32 devices in a mesh: space: 8 (over z, y), tm: 4 (over x, core).
Axes of the slice: x: 2, y: 2, z: 4, core: 2. Of those that a mesh axis runs over, the one named last changes fastest.
Arguments:
- innovations: bfloat16 [12, 32, 768, 1536], P('tm', None, 'space'), may hold values from -6 to 6
- obs_counts: int32 [12, 192, 384], P('tm', 'space'), may hold values from 0 to 3
- diffusion: float32 [32, 192, 384], P(None, 'space'), may hold values from 0.01 to 0.1
- courant: float32 [32, 192, 384], P(None, 'space'), may hold values from 0 to 0.4
Outputs:
- increment: float32 [32, 768, 1536], P('tm', 'space')
- residual: float32 [32, 192, 384], P('tm', 'space')
The draws below stay inside these ranges and needn't reach their ends.
All inputs are finite; a program needn't handle non-finite values.
Results may differ from the reference program's by a relative error of at most 0.0003.
Values sent between devices are 32-bit elements; how exact they have to be, the bound alone decides.
A program may use at most 384 MiB of HBM per device.

```python
import math
import jax
import jax.numpy as jnp
from jax import lax

NLAT_F = 768
NLON_F = 1536
LEV = 32
ITERS = 3
NLAT = 192
NLON = 384
STEPS = 12


def touch_ends(entries, rng, smallest, high):
    spot = [jax.random.randint(jax.random.fold_in(rng, axis), (), 0, length) for axis, length in enumerate(entries.shape)]
    main_axis = entries.shape.index(max(entries.shape))
    next_to = spot[:main_axis] + [(spot[main_axis] + 1) % entries.shape[main_axis]] + spot[main_axis + 1:]
    return entries.at[tuple(spot)].set(smallest).at[tuple(next_to)].set(high)


def levels(rng, dims, split, smallest, high):
    factor_of, own = 1.0, jax.random.fold_in(rng, 6)
    for axis_at, parts in split:
        draws = jnp.exp(jax.random.uniform(jax.random.fold_in(own, axis_at), (parts,), jnp.float32, smallest / len(split), high / len(split)))
        factor_of = factor_of * jnp.repeat(draws, dims[axis_at] // parts).reshape([-1 if axis == axis_at else 1 for axis in range(len(dims))])
    return factor_of


def bell_draw(key, shape, spread, limit, cuts=(), held_as=jnp.bfloat16):
    entries = spread * jax.random.normal(key, shape, jnp.float32)
    if cuts:
        entries = entries * levels(key, shape, cuts, -0.22, 0.18)
    return jnp.clip(entries, -limit, limit).astype(held_as)


def setup_inputs(seed: int = 0) -> dict:
    key_list = jax.random.split(jax.random.key(seed), 5)
    innovations = bell_draw(key_list[0], (STEPS, LEV, NLAT_F, NLON_F), 1.0, 6.0, ((0, 4), (2, 8)))
    obs_counts = touch_ends(jax.random.randint(key_list[1], (STEPS, NLAT, NLON), 0, 4), jax.random.fold_in(key_list[1], 1), 0, 3).astype(jnp.int32)
    diffusion = jnp.clip(jnp.exp(math.log(0.1) - 2.3025851 * jax.random.uniform(key_list[2], (LEV, NLAT, NLON), jnp.float32) ** levels(key_list[2], (LEV, NLAT, NLON), ((1, 8),), -0.2, 0.2)), 0.01, 0.1)
    courant = jnp.clip(0.4 * jax.random.uniform(key_list[3], (LEV, NLAT, NLON), jnp.float32) ** levels(key_list[3], (LEV, NLAT, NLON), ((1, 8),), -0.2, 0.2), 0.0, 0.4)
    return {"innovations": innovations, "obs_counts": obs_counts, "diffusion": diffusion, "courant": courant}


def laplace(state_field):
    padded = jnp.pad(state_field, ((0, 0), (1, 1), (0, 0)))
    return padded[:, 2:, :] + padded[:, :-2, :] + jnp.roll(state_field, 1, 2) + jnp.roll(state_field, -1, 2) - 4.0 * state_field


def tangent(state_field, diffusion, courant):
    return state_field + diffusion * laplace(state_field) - courant * (state_field - jnp.roll(state_field, 1, 2))


def adjoint(state_field, diffusion, courant):
    carried = courant * state_field
    return state_field + laplace(diffusion * state_field) - carried + jnp.roll(carried, -1, 2)


def restrict(block_field):
    coarse = block_field.astype(jnp.float32).reshape(LEV, NLAT_F // 4, 4, NLON_F // 4, 4)
    return jnp.mean(coarse, axis=(2, 4))


def reference(innovations, obs_counts, diffusion, courant):
    weights = obs_counts.astype(jnp.float32)[:, None]
    forcing = weights * lax.map(restrict, innovations)

    def forward(state_field):
        records = []
        for step_no in range(STEPS):
            records.append(weights[step_no] * state_field)
            if step_no + 1 < STEPS:
                state_field = tangent(state_field, diffusion, courant)
        return jnp.stack(records)

    def backward(terms):
        current = terms[STEPS - 1]
        for step_no in range(STEPS - 2, -1, -1):
            current = terms[step_no] + adjoint(current, diffusion, courant)
        return current

    rhs_field = backward(forcing)
    control = jnp.zeros_like(rhs_field)
    residual = rhs_field
    direction = rhs_field
    norm_now = jnp.sum(residual * residual)
    for iter_no in range(ITERS):
        hessian_image = direction + backward(forward(direction))
        step_len = norm_now / jnp.sum(direction * hessian_image)
        control = control + step_len * direction
        residual = residual - step_len * hessian_image
        if iter_no + 1 < ITERS:
            norm_next = jnp.sum(residual * residual)
            direction = residual + (norm_next / norm_now) * direction
            norm_now = norm_next
    increment = jnp.repeat(jnp.repeat(control, 4, axis=1), 4, axis=2)
    return increment, residual
```

```python
import functools

import jax
import jax.numpy as jnp
from jax import lax
from jax.experimental import pallas as pl
from jax.experimental.pallas import tpu as pltpu
from jax.sharding import PartitionSpec as P

ITERS = 3
F32 = jnp.float32
BF16 = jnp.bfloat16
MESH = pl.DeviceIdType.MESH
SLOTS = 3
COARSE = 4


def adjoint_rows(src, co, low, count, emit):
    co_a, co_b, co_d = co
    cols = src.shape[-1]
    before = co_d[low - 1] * src[low - 1]
    y = src[low]
    here = co_d[low] * y
    for row in range(low, low + count):
        y_next = src[row + 1]
        after = co_d[row + 1] * y_next
        value = (
            co_a[row] * y
            + (before + after)
            + pltpu.roll(here, 1, 1)
            + pltpu.roll(co_b[row] * y, cols - 1, 1)
        )
        emit(row, value)
        before, here, y = here, after, y_next


def shift_groups(value, by):
    groups = value.shape[0]
    at = lax.broadcasted_iota(jnp.int32, value.shape, 0)
    outside = 0 if by == 1 else groups - 1
    return jnp.where(at == outside, 0.0, pltpu.roll(value, by % groups, 0))


def level_forward(src, dst, co):
    co_a, co_b, co_d = co
    rows, cols = src.shape[0], src.shape[-1]
    above = shift_groups(src[rows - 1], 1)
    here = first = src[0]
    for row in range(rows):
        below = src[row + 1] if row + 1 < rows else shift_groups(first, -1)
        dst[row] = (
            co_a[row] * here
            + co_d[row] * (above + below + pltpu.roll(here, cols - 1, 1))
            + co_b[row] * pltpu.roll(here, 1, 1)
        )
        above, here = here, below


def level_backward(src, dst, state, weight, co):
    co_a, co_b, co_d = co
    rows, cols = src.shape[0], src.shape[-1]
    above = shift_groups(co_d[rows - 1] * src[rows - 1], 1)
    y = src[0]
    here = first = co_d[0] * y
    for row in range(rows):
        y_next = src[row + 1] if row + 1 < rows else None
        below = shift_groups(first, -1) if y_next is None else co_d[row + 1] * y_next
        dst[row] = (
            co_a[row] * y
            + (above + below)
            + pltpu.roll(here, 1, 1)
            + pltpu.roll(co_b[row] * y, cols - 1, 1)
            + weight[row] * state[row]
        )
        above, here, y = here, below, y_next


def assimilate_kernel(
    n_space,
    n_tm,
    inn,
    obs,
    diff,
    cour,
    control,
    residual,
    inbuf,
    summed,
    turned,
    fields,
    counts,
    forcing,
    p_a,
    p_b,
    p_d,
    p_lam,
    p_send,
    p_recv,
    edge_src,
    edge_recv,
    halo_src,
    halo_recv,
    c_a,
    c_b,
    c_d,
    lam_0,
    lam_1,
    l_send,
    l_recv,
    f_recv,
    v_a,
    v_b,
    v_d,
    states,
    wts,
    adj_0,
    adj_1,
    resid,
    r_send,
    r_recv,
    red_src,
    red_tm,
    red_space,
    steps_ab,
    in_sems,
    loc_sems,
    w_send,
    w_recv,
    core_recv,
    edge_sems,
    halo_sems,
    f_sems,
    p_sems,
    l_sems,
    r_sems,
    red_tm_sems,
    red_space_sems,
):
    steps = forcing.shape[0]
    part, cols = forcing.shape[2:]
    rows = resid.shape[0]
    fine_rows = inbuf.shape[2]
    total = steps * n_tm
    halo = total - 1
    reach = steps - 1
    margin = reach + 1
    pad = halo + 1
    span = l_send.shape[1] // n_space
    pieces = cols // 128
    own_rows = steps * rows
    wide = 128 * COARSE
    n_z, n_x = n_space // 2, n_tm // 2
    place = lax.axis_index("space")
    section = lax.axis_index("tm")
    z, y = lax.div(place, 2), lax.rem(place, 2)
    x, core = lax.div(section, 2), lax.rem(section, 2)
    above, below = place - 1, place + 1
    has_above, has_below = place > 0, place < n_space - 1
    tm_peers = [lax.rem(section + k, n_tm) for k in range(1, n_tm)]
    space_peers = [lax.rem(place + k, n_space) for k in range(1, n_space)]
    lanes = [slice(piece * 128, (piece + 1) * 128) for piece in range(pieces)]

    def to(axis, peer):
        return {"device_id": {axis: peer}, "device_id_type": MESH}

    def remote(src, dst, send_sem, recv_sem, axis, peer):
        return pltpu.make_async_remote_copy(
            src_ref=src, dst_ref=dst, send_sem=send_sem, recv_sem=recv_sem, **to(axis, peer)
        )

    def slab(ref, index, size):
        return ref.at[:, pl.ds(pl.multiple_of(index * size, 8), size), :]

    def group_of(turn):
        d_x = lax.rem(lax.div(turn, 2) + 1, n_x)
        d_core = lax.rem(turn + 1, 2)
        return lax.rem(x + d_x, n_x) * 2 + lax.rem(core + d_core, 2)

    def block_copy(k):
        turn, t, slot = lax.div(k, steps), lax.rem(k, steps), lax.rem(k, SLOTS)
        return pltpu.make_async_copy(
            inn.at[t, pl.ds(group_of(turn) * part, part)], inbuf.at[slot], in_sems.at[slot]
        )

    own_counts = slab(counts.at[section], place, own_rows)
    local = []
    for piece in range(pieces):
        local.append(
            pltpu.make_async_copy(obs.at[:, lanes[piece]], own_counts.at[piece], loc_sems.at[piece, 0])
        )
        for k, field in enumerate((diff, cour)):
            local.append(
                pltpu.make_async_copy(
                    field.at[:, lanes[piece]], fields.at[k, piece], loc_sems.at[piece, 1 + k]
                )
            )
    for copy in local:
        copy.start()
    for k in range(SLOTS):
        block_copy(jnp.int32(k)).start()

    edge_recv[...] = jnp.zeros_like(edge_recv)
    halo_recv[...] = jnp.zeros_like(halo_recv)
    barrier = pltpu.get_barrier_semaphore()
    for peer in tm_peers:
        pl.semaphore_signal(barrier, inc=1, **to("tm", peer))
    for peer in space_peers:
        pl.semaphore_signal(barrier, inc=1, **to("space", peer))

    forcing[...] = jnp.zeros_like(forcing)
    p_lam[...] = jnp.zeros_like(p_lam)
    for ref in (p_a, p_b, p_d, c_a, c_b, c_d, lam_0, lam_1):
        ref[...] = jnp.zeros_like(ref)
    states[0] = jnp.zeros_like(states[0])

    for copy in local:
        copy.wait()

    def by_level(k, group, row, piece):
        return fields[k, piece, pl.ds(group * (part * rows) + row, part, stride=rows), :]

    for k in range(2):
        for piece in range(pieces):
            at = lanes[piece]
            for side, row in enumerate((0, rows - 1)):
                for group in range(n_tm):
                    edge_src[k, side, group, :, at] = by_level(k, group, row, piece)
            for side, first in enumerate((0, rows - halo)):
                for row in range(halo):
                    halo_src[k, side, row, :, at] = by_level(k, section, first + row, piece)

    pl.semaphore_wait(barrier, n_tm - 1 + n_space - 1)

    def pair(src, dst, sems):
        up = remote(src.at[0], dst.at[1], sems.at[0, 0], sems.at[1, 0], "space", above)
        down = remote(src.at[1], dst.at[0], sems.at[0, 1], sems.at[1, 1], "space", below)
        return [(has_above, has_below, up), (has_below, has_above, down)]

    def start(copies):
        for sends, _, copy in copies:
            pl.when(sends)(copy.start)

    def finish(copies):
        for sends, receives, copy in copies:
            pl.when(sends)(copy.wait_send)
            pl.when(receives)(copy.wait_recv)

    edge_copies = pair_copies = []
    edge_copies = pair(edge_src.at[0], edge_recv.at[0], edge_sems.at[0])
    edge_copies += pair(edge_src.at[1], edge_recv.at[1], edge_sems.at[1])
    start(edge_copies)

    w_copies = []
    y_peer = z * 2 + (1 - y)
    x_peers = [lax.rem(x + d_x, n_x) * 2 + core for d_x in range(1, n_x)]
    line = [lax.rem(z + k, n_z) for k in range(n_z)]
    near = [at * 2 + y for at in line]
    far = [at * 2 + (1 - y) for at in line]
    half = n_z // 2

    def count_send(owner, owner_place, axis, peer):
        block = slab(counts.at[owner], owner_place, own_rows)
        copy = remote(
            block, block, w_send.at[len(w_copies)], w_recv.at[owner, owner_place], axis, peer
        )
        copy.start()
        w_copies.append(copy)

    def count_wait(owner, owner_place):
        block = slab(counts.at[owner], owner_place, own_rows)
        remote(block, block, w_send.at[0], w_recv.at[owner, owner_place], "space", y_peer).wait_recv()

    def count_spread(owner, owner_place, along_y=True, along_x=True):
        if along_y:
            count_send(owner, owner_place, "space", y_peer)
        if along_x:
            for peer in x_peers:
                count_send(owner, owner_place, "tm", peer)

    for peer in near[1:]:
        count_send(section, place, "space", peer)
    count_spread(section, place)

    halo_copies = pair(halo_src.at[0], halo_recv.at[0], halo_sems.at[0])
    halo_copies += pair(halo_src.at[1], halo_recv.at[1], halo_sems.at[1])
    start(halo_copies)

    f_copies = []
    for k in range(2):
        for j, peer in enumerate(space_peers):
            copy = remote(
                slab(fields.at[k], section * part + peer, rows),
                slab(f_recv.at[k], place, rows),
                f_sems.at[k, 0, j],
                f_sems.at[k, 1, place],
                "space",
                peer,
            )
            copy.start()
            f_copies.append(copy)
        slab(f_recv.at[k], place, rows)[...] = slab(fields.at[k], section * part + place, rows)[...]

    pick = jnp.where(
        lax.broadcasted_iota(jnp.int32, (wide, 128), 0) // COARSE
        == lax.broadcasted_iota(jnp.int32, (wide, 128), 1),
        1.0 / (COARSE * COARSE),
        0.0,
    ).astype(BF16)

    def restrict(turn, t):
        k = turn * steps + t
        block_copy(k).wait()
        slot = lax.rem(k, SLOTS)
        for piece in range(pieces):
            block = inbuf[slot, :, :, piece * wide : (piece + 1) * wide].reshape(part * fine_rows, wide)
            summed[piece] = jnp.dot(block, pick, preferred_element_type=F32)
        pl.when(k + SLOTS < total)(lambda: block_copy(k + SLOTS).start())
        for piece in range(pieces):
            first = pl.multiple_of(place * own_rows + t * rows, 8)
            scale = counts[section, piece, pl.ds(first, rows), :].astype(F32)
            for level in range(part):
                value = summed[piece, pl.ds(level * fine_rows, rows, stride=COARSE), :]
                for sub in range(1, COARSE):
                    value += summed[piece, pl.ds(level * fine_rows + sub, rows, stride=COARSE), :]
                turned[piece, pl.ds(level, rows, stride=part), :] = value * scale
            forcing[t, pl.ds(margin, rows), :, lanes[piece]] = turned[piece].reshape(rows, part, 128)

    def put(co, row, d, c, at=slice(None), inside=None):
        a = 1.0 - 4.0 * d - c
        if inside is not None:
            a = jnp.where(inside, a, 0.0)
        co[0][row, :, at] = a
        co[1][row, :, at] = d + c
        co[2][row, :, at] = d

    p_co = (p_a, p_b, p_d)
    reach_rows = rows + 2 * reach

    def carry_back(turn):
        group = group_of(turn)
        for row in range(rows):
            for piece in range(pieces):
                d, c = by_level(0, group, row, piece), by_level(1, group, row, piece)
                put(p_co, margin + row, d, c, lanes[piece])
        put(p_co, margin - 1, edge_recv[0, 0, group], edge_recv[1, 0, group], inside=has_above)
        put(p_co, margin + rows, edge_recv[0, 1, group], edge_recv[1, 1, group], inside=has_below)
        now = forcing.at[steps - 1]
        for k in range(1, steps):
            t = steps - 1 - k

            def emit(row, value, k=k, t=t):
                value = value + forcing[t, row]
                if k < steps - 1:
                    p_lam[k % 2, row] = value
                else:
                    p_send[turn, row - (margin - reach)] = value

            adjoint_rows(now, p_co, margin - reach, reach_rows, emit)
            now = p_lam.at[k % 2]

    def p_copy(turn):
        return remote(
            p_send.at[turn],
            p_recv.at[section],
            p_sems.at[0, turn],
            p_sems.at[1, section],
            "tm",
            group_of(turn),
        )

    def one_turn(turn, carry):
        def one(t, carry):
            restrict(turn, t)
            return carry

        lax.fori_loop(0, steps, one, 0)
        pl.when(turn == 0)(lambda: finish(edge_copies))
        carry_back(turn)
        pl.when(turn < n_tm - 1)(lambda: p_copy(turn).start())
        return carry

    middle = n_tm // 2
    lax.fori_loop(0, middle, one_turn, 0)
    for at in near[1:]:
        count_wait(section, at)
        count_spread(section, at)
    lax.fori_loop(middle, n_tm, one_turn, 0)
    for k in range(n_z):
        if k >= half:
            count_wait(section, far[k])
            count_spread(section, far[k], along_y=False)
        else:
            for peer in x_peers:
                count_wait(peer, near[k])
                count_spread(peer, near[k], along_x=False)

    finish(halo_copies)
    c_co = (c_a, c_b, c_d)
    for row in range(rows):
        for piece in range(pieces):
            d, c = by_level(0, section, row, piece), by_level(1, section, row, piece)
            put(c_co, pad + row, d, c, lanes[piece])
    for row in range(halo):
        put(c_co, pad - halo + row, halo_recv[0, 0, row], halo_recv[1, 0, row], inside=has_above)
        put(c_co, pad + rows + row, halo_recv[0, 1, row], halo_recv[1, 1, row], inside=has_below)
    p_recv[section] = p_send[n_tm - 1]
    for k, peer in enumerate(tm_peers):
        p_copy(jnp.int32(k)).wait_send()
        remote(
            p_send.at[0], p_recv.at[peer], p_sems.at[0, 0], p_sems.at[1, peer], "tm", peer
        ).wait_recv()
    lam = [lam_0, lam_1]
    for row in range(reach_rows):
        lam_0[pad - reach + row] = p_recv[n_tm - 1, row]
    slot, grown = 0, reach
    for other in range(n_tm - 2, -1, -1):
        for k in range(steps):
            grown += 1
            last = other == 0 and k == steps - 1

            def emit(row, value, k=k, other=other, slot=slot, last=last):
                inside = row - (pad - reach)
                if k == steps - 1 and 0 <= inside < reach_rows:
                    value = value + p_recv[other, inside]
                if last:
                    for piece in range(pieces):
                        at = pl.ds(row - (pad - halo), part, stride=span)
                        l_send[piece, at, :] = value[:, lanes[piece]]
                else:
                    lam[1 - slot][row] = value

            adjoint_rows(lam[slot], c_co, pad - grown, rows + 2 * grown, emit)
            slot = 1 - slot

    l_copies = []
    for j, peer in enumerate(space_peers):
        copy = remote(
            slab(l_send, peer, span),
            slab(l_recv, place, span),
            l_sems.at[0, j],
            l_sems.at[1, place],
            "space",
            peer,
        )
        copy.start()
        l_copies.append(copy)
    slab(l_recv, place, span)[...] = slab(l_send, place, span)[...]

    for k in range(n_z):
        if k < half:
            count_wait(section, far[k])
        for peer in x_peers:
            if k >= half:
                count_wait(peer, near[k])
            count_wait(peer, far[k])
    first_copies = len(w_copies)
    mine = [lax.rem(x + d_x, n_x) * 2 + core for d_x in range(n_x)]
    theirs = [lax.rem(x + d_x, n_x) * 2 + (1 - core) for d_x in range(n_x)]
    for owner in mine:
        block = counts.at[owner]
        copy = remote(
            block, block, w_send.at[len(w_copies)], core_recv.at[owner], "tm", x * 2 + (1 - core)
        )
        copy.start()
        w_copies.append(copy)

    for k in range(2):
        for peer in space_peers:
            block = slab(f_recv.at[k], peer, rows)
            remote(block, block, f_sems.at[k, 0, 0], f_sems.at[k, 1, peer], "space", peer).wait_recv()
    v_co = (v_a, v_b, v_d)
    for row in range(rows):
        for piece in range(pieces):
            at = pl.ds(row, n_space, stride=rows)
            put(v_co, row, f_recv[0, piece, at, :], f_recv[1, piece, at, :], lanes[piece])

    def spread_counts(owner):
        def one(t, carry):
            for row in range(rows):
                for piece in range(pieces):
                    value = counts[owner, piece, pl.ds(t * rows + row, n_space, stride=own_rows), :]
                    wts[owner * steps + t, row, :, lanes[piece]] = value.astype(F32)
            return carry

        lax.fori_loop(0, steps, one, 0)

    for owner in mine:
        spread_counts(owner)
    for owner in theirs:
        block = counts.at[owner]
        remote(
            block, block, w_send.at[0], core_recv.at[owner], "tm", x * 2 + (1 - core)
        ).wait_recv()
        spread_counts(owner)

    for j, peer in enumerate(space_peers):
        block = slab(l_recv, peer, span)
        remote(block, block, l_sems.at[0, 0], l_sems.at[1, peer], "space", peer).wait_recv()

    def received(row, piece):
        return l_recv[piece, pl.ds(row, n_space, stride=span), :]

    for row in range(rows):
        for piece in range(pieces):
            value = received(halo + row, piece)
            from_below = row - (rows - halo)
            if from_below >= 0:
                value = value + shift_groups(received(from_below, piece), -1)
            if row < halo:
                value = value + shift_groups(received(halo + rows + row, piece), 1)
            resid[row, :, lanes[piece]] = value
            r_send[0, piece, pl.ds(row, n_space, stride=rows), :] = value

    def residual_copy(k, j, peer):
        return remote(
            slab(r_send.at[k], peer, rows),
            slab(r_recv.at[k], place, rows),
            r_sems.at[k, 0, j],
            r_sems.at[k, 1, place],
            "space",
            peer,
        )

    def send_residual(k):
        for j, peer in enumerate(space_peers):
            residual_copy(k, j, peer).start()
        slab(r_recv.at[k], place, rows)[...] = slab(r_send.at[k], place, rows)[...]

    def reduce_over(me, peers, axis, count, tile, src, slots, sems):
        src[...] = tile
        slots[me] = tile
        copies = [
            remote(src, slots.at[me], sems.at[0, j], sems.at[1, me], axis, peer)
            for j, peer in enumerate(peers)
        ]
        for copy in copies:
            copy.start()
        for j, peer in enumerate(peers):
            copies[j].wait_send()
            remote(src, slots.at[peer], sems.at[0, j], sems.at[1, peer], axis, peer).wait_recv()
        value = slots[0]
        for j in range(1, count):
            value = value + slots[j]
        return value

    def reduce_all(k, partials):
        at = lax.broadcasted_iota(jnp.int32, (8, 128), 0)
        tile = jnp.zeros((8, 128), F32)
        for j, partial in enumerate(partials):
            folded = partial[:, lanes[0]]
            for piece in range(1, pieces):
                folded = folded + partial[:, lanes[piece]]
            tile = jnp.where(at == j, jnp.sum(folded, axis=0, keepdims=True), tile)
        tile = reduce_over(
            section, tm_peers, "tm", n_tm, tile, red_src.at[k, 0], red_tm.at[k], red_tm_sems.at[k]
        )
        tile = reduce_over(
            place,
            space_peers,
            "space",
            n_space,
            tile,
            red_src.at[k, 1],
            red_space.at[k],
            red_space_sems.at[k],
        )
        sums = jnp.sum(tile, axis=1, keepdims=True)
        return [sums[j : j + 1] for j in range(len(partials))]

    adj = [adj_0, adj_1]

    def iterate(k, beta):
        send_residual(k)
        for row in range(rows):
            states[0, row] = resid[row] + beta * states[0, row]
        for t in range(1, total):
            level_forward(states.at[t - 1], states.at[t], v_co)
        for row in range(rows):
            adj_0[row] = wts[total - 1, row] * states[total - 1, row]
        slot = 0
        for t in range(total - 2, -1, -1):
            level_backward(adj[slot], adj[1 - slot], states.at[t], wts.at[t], v_co)
            slot = 1 - slot
        image = adj[slot]
        rr = dq = rq = qq = jnp.zeros((n_space, cols), F32)
        for row in range(rows):
            d, r = states[0, row], resid[row]
            q = d + image[row]
            image[row] = q
            rr, dq, rq, qq = rr + r * r, dq + d * q, rq + r * q, qq + q * q
        rr, dq, rq, qq = reduce_all(k, (rr, dq, rq, qq))
        alpha = rr / dq
        for row in range(rows):
            r = resid[row] - alpha * image[row]
            resid[row] = r
            for piece in range(pieces):
                r_send[k + 1, piece, pl.ds(row, n_space, stride=rows), :] = r[:, lanes[piece]]
        steps_ab[k, 0] = jnp.broadcast_to(alpha, (8, 128))
        steps_ab[k, 1] = jnp.broadcast_to(beta, (8, 128))
        return (rr - 2.0 * alpha * rq + alpha * alpha * qq) / rr

    lax.fori_loop(0, ITERS, iterate, jnp.zeros((1, 1), F32))
    send_residual(ITERS)

    factors = [None] * ITERS
    factor = None
    for k in range(ITERS - 1, -1, -1):
        alpha = steps_ab[k, 0, 0:1, :]
        factor = alpha if factor is None else alpha + steps_ab[k + 1, 1, 0:1, :] * factor
        factors[k] = factor

    def residual_arrived(k):
        for peer in space_peers:
            block = slab(r_recv.at[k], peer, rows)
            remote(block, block, r_sems.at[k, 0, 0], r_sems.at[k, 1, peer], "space", peer).wait_recv()

    for k in range(ITERS):
        residual_arrived(k)
    for piece in range(pieces):
        value = factors[0] * r_recv[0, piece]
        for k in range(1, ITERS):
            value = value + factors[k] * r_recv[k, piece]
        control[piece] = value
    residual_arrived(ITERS)
    residual[...] = r_recv[ITERS]

    for k in range(ITERS + 1):
        for j, peer in enumerate(space_peers):
            residual_copy(k, j, peer).wait_send()
    for copy in w_copies + f_copies + l_copies:
        copy.wait_send()


def assimilate_call(innovations, obs_counts, diffusion, courant, n_space, n_tm):
    steps, levels, fine_rows, fine_cols = innovations.shape
    part = levels // n_tm
    rows, cols = fine_rows // COARSE, fine_cols // COARSE
    pieces = cols // 128
    total = steps * n_tm
    halo = total - 1
    reach = steps - 1
    padded = rows + 2 * (reach + 1)
    ext = rows + 2 * (halo + 1)
    span = -(-(rows + 2 * halo) // 8) * 8
    row = (part, cols)
    n_x, n_z = n_tm // 2, n_space // 2
    sends = n_z - 1 + n_z * n_x + n_z * n_x + n_x
    dma = pltpu.SemaphoreType.DMA
    shapes = [
        pltpu.VMEM((SLOTS, part, fine_rows, fine_cols), BF16),
        pltpu.VMEM((pieces, part * fine_rows, 128), F32),
        pltpu.VMEM((pieces, part * rows, 128), F32),
        pltpu.VMEM((2, pieces, levels * rows, 128), F32),
        pltpu.VMEM((n_tm, pieces, n_space * steps * rows, 128), jnp.int32),
        pltpu.VMEM((steps, padded, *row), F32),
        pltpu.VMEM((padded, *row), F32),
        pltpu.VMEM((padded, *row), F32),
        pltpu.VMEM((padded, *row), F32),
        pltpu.VMEM((2, padded, *row), F32),
        pltpu.VMEM((n_tm, rows + 2 * reach, *row), F32),
        pltpu.VMEM((n_tm, rows + 2 * reach, *row), F32),
        pltpu.VMEM((2, 2, n_tm, *row), F32),
        pltpu.VMEM((2, 2, n_tm, *row), F32),
        pltpu.VMEM((2, 2, halo, *row), F32),
        pltpu.VMEM((2, 2, halo, *row), F32),
        pltpu.VMEM((ext, *row), F32),
        pltpu.VMEM((ext, *row), F32),
        pltpu.VMEM((ext, *row), F32),
        pltpu.VMEM((ext, *row), F32),
        pltpu.VMEM((ext, *row), F32),
        pltpu.VMEM((pieces, n_space * span, 128), F32),
        pltpu.VMEM((pieces, n_space * span, 128), F32),
        pltpu.VMEM((2, pieces, n_space * rows, 128), F32),
        pltpu.VMEM((rows, n_space, cols), F32),
        pltpu.VMEM((rows, n_space, cols), F32),
        pltpu.VMEM((rows, n_space, cols), F32),
        pltpu.VMEM((total, rows, n_space, cols), F32),
        pltpu.VMEM((total, rows, n_space, cols), F32),
        pltpu.VMEM((rows, n_space, cols), F32),
        pltpu.VMEM((rows, n_space, cols), F32),
        pltpu.VMEM((rows, n_space, cols), F32),
        pltpu.VMEM((ITERS + 1, pieces, n_space * rows, 128), F32),
        pltpu.VMEM((ITERS + 1, pieces, n_space * rows, 128), F32),
        pltpu.VMEM((ITERS, 2, 8, 128), F32),
        pltpu.VMEM((ITERS, n_tm, 8, 128), F32),
        pltpu.VMEM((ITERS, n_space, 8, 128), F32),
        pltpu.VMEM((ITERS, 2, 8, 128), F32),
        dma((SLOTS,)),
        dma((pieces, 3)),
        dma((sends,)),
        dma((n_tm, n_space)),
        dma((n_tm,)),
        dma((2, 2, 2)),
        dma((2, 2, 2)),
        dma((2, 2, n_space)),
        dma((2, n_tm)),
        dma((2, n_space)),
        dma((ITERS + 1, 2, n_space)),
        dma((ITERS, 2, n_tm)),
        dma((ITERS, 2, n_space)),
    ]
    out = jax.ShapeDtypeStruct((pieces, part * rows, 128), F32)
    return pl.pallas_call(
        functools.partial(assimilate_kernel, n_space, n_tm),
        out_shape=[out] * 2,
        in_specs=[pl.BlockSpec(memory_space=pl.ANY)] * 4,
        out_specs=[pl.BlockSpec(memory_space=pltpu.VMEM)] * 2,
        scratch_shapes=shapes,
        compiler_params=pltpu.CompilerParams(
            collective_id=0, has_side_effects=True, vmem_limit_bytes=60 * 2**20
        ),
        name="assimilate",
    )(
        innovations,
        obs_counts.reshape(steps * rows, cols),
        diffusion.reshape(levels * rows, cols),
        courant.reshape(levels * rows, cols),
    )


def expand_kernel(control, residual, increment, residual_out, repeated):
    rows = residual_out.shape[1]
    pieces = control.shape[0]
    wide = 128 * COARSE
    pick = jnp.where(
        lax.broadcasted_iota(jnp.int32, (128, wide), 1) // COARSE
        == lax.broadcasted_iota(jnp.int32, (128, wide), 0),
        1.0,
        0.0,
    ).astype(BF16)
    for piece in range(pieces):
        residual_out[0, :, piece * 128 : (piece + 1) * 128] = residual[piece]
        values = control[piece]
        for sub in range(COARSE):
            repeated[piece, pl.ds(sub, rows, stride=COARSE), :] = values
        rest = repeated[piece]
        total = None
        for _ in range(3):
            head = rest.astype(BF16)
            rest = rest - head.astype(F32)
            spread = jnp.dot(head, pick, preferred_element_type=F32)
            total = spread if total is None else total + spread
        increment[0, :, piece * wide : (piece + 1) * wide] = total


def expand_call(control, residual, part):
    pieces, count, _ = control.shape
    rows, cols = count // part, pieces * 128
    level = pl.BlockSpec((pieces, rows, 128), lambda l: (0, l, 0))
    return pl.pallas_call(
        expand_kernel,
        grid=(part,),
        in_specs=[level, level],
        out_specs=[
            pl.BlockSpec((1, rows * COARSE, cols * COARSE), lambda l: (l, 0, 0)),
            pl.BlockSpec((1, rows, cols), lambda l: (l, 0, 0)),
        ],
        out_shape=[
            jax.ShapeDtypeStruct((part, rows * COARSE, cols * COARSE), F32),
            jax.ShapeDtypeStruct((part, rows, cols), F32),
        ],
        scratch_shapes=[pltpu.VMEM((pieces, rows * COARSE, 128), F32)],
        compiler_params=pltpu.CompilerParams(vmem_limit_bytes=32 * 2**20),
        name="expand",
    )(control, residual)


def padded_2(cells, sides, width):
    for axis, dim in sides:
        count = lax.axis_size(axis)
        ends = count - 1
        head = lax.slice_in_dim(cells, 0, width, axis=dim)
        tail = lax.slice_in_dim(cells, cells.shape[dim] - width, cells.shape[dim], axis=dim)
        cells = jnp.concatenate(
            [
                lax.ppermute(tail, axis, [(i, (i + 1) % count) for i in range(ends)]),
                cells,
                lax.ppermute(head, axis, [((i + 1) % count, i) for i in range(ends)]),
            ],
            axis=dim,
        )
    return cells


def laplace_rows(padded, state_field):
    return (
        padded[:, 2:, :]
        + padded[:, :-2, :]
        + jnp.roll(state_field, 1, 2)
        + jnp.roll(state_field, -1, 2)
        - 4.0 * state_field
    )


def tangent(state_field, diffusion, courant):
    padded = padded_2(state_field, (("space", 1),), 1)
    return (
        state_field
        + diffusion * laplace_rows(padded, state_field)
        - courant * (state_field - jnp.roll(state_field, 1, 2))
    )


def adjoint(state_field, diffusion, courant):
    carried = courant * state_field
    spread = diffusion * state_field
    padded = padded_2(spread, (("space", 1),), 1)
    return state_field + laplace_rows(padded, spread) - carried + jnp.roll(carried, -1, 2)


def level_squares(residual):
    return lax.psum(jnp.sum(residual * residual), ("space", "tm"))


def level_curve(direction, hessian_image):
    return lax.psum(jnp.sum(direction * hessian_image), ("space", "tm"))


def solve_inner(rhs_field, hessian_part, norm_fn, curve_fn):
    control = jnp.zeros_like(rhs_field)
    residual = rhs_field
    direction = rhs_field
    norm_now = norm_fn(residual)
    for iter_no in range(ITERS):
        hessian_image = direction + hessian_part(direction)
        step_len = norm_now / curve_fn(direction, hessian_image)
        control = control + step_len * direction
        residual = residual - step_len * hessian_image
        if iter_no + 1 < ITERS:
            norm_next = norm_fn(residual)
            direction = residual + norm_next / norm_now * direction
            norm_now = norm_next
    return (control, residual)


def on_device(innovations, obs_counts, diffusion, courant):
    step_dev = obs_counts.shape[0]
    n_sections = lax.axis_size("tm")
    section_pos = lax.axis_index("tm")
    total_steps = step_dev * n_sections
    weights = obs_counts.astype(jnp.float32)[:, None]
    levels, fine_rows, fine_cols = (
        innovations.shape[1],
        innovations.shape[2],
        innovations.shape[3],
    )
    lev_part = levels // n_sections
    rows, cols = fine_rows // COARSE, fine_cols // COARSE
    n_space = lax.axis_size("space")
    tiled = lev_part == 8 and rows % 8 == 0 and cols % 128 == 0
    paired = n_space == lev_part and n_sections % 2 == 0
    if tiled and paired and rows >= total_steps - 1:
        solved = assimilate_call(innovations, obs_counts, diffusion, courant, n_space, n_sections)
        return tuple(expand_call(*solved, lev_part))
    blocks = innovations.reshape(step_dev, levels, fine_rows // 4, 4, fine_cols // 4, 4).astype(
        jnp.float32
    )
    forcing = weights * jnp.mean(blocks, axis=(3, 5))
    all_weights = lax.all_gather(obs_counts, "tm", axis=0, tiled=True).astype(jnp.float32)[:, None]
    all_forcing = lax.all_to_all(forcing, "tm", split_axis=1, concat_axis=0, tiled=True)
    diff_part = lax.dynamic_slice_in_dim(diffusion, section_pos * lev_part, lev_part, 0)
    cour_part = lax.dynamic_slice_in_dim(courant, section_pos * lev_part, lev_part, 0)

    def level_back(terms):
        current = terms[total_steps - 1]
        for step_no in range(total_steps - 2, -1, -1):
            current = terms[step_no] + adjoint(current, diff_part, cour_part)
        return current

    def level_hess(state_field):
        records = []
        for step_no in range(total_steps):
            records.append(all_weights[step_no] * state_field)
            if step_no + 1 < total_steps:
                state_field = tangent(state_field, diff_part, cour_part)
        return level_back(jnp.stack(records))

    control, residual = solve_inner(level_back(all_forcing), level_hess, level_squares, level_curve)
    increment = jnp.repeat(jnp.repeat(control, 4, axis=1), 4, axis=2)
    return (increment, residual)


def solution(mesh):
    placed = (
        P("tm", None, "space", None),
        P("tm", "space", None),
        P(None, "space", None),
        P(None, "space", None),
    )
    return jax.shard_map(
        on_device,
        mesh=mesh,
        in_specs=placed,
        out_specs=(P("tm", "space", None), P("tm", "space", None)),
        check_vma=False,
    )
```

```python
import functools

import jax
import jax.numpy as jnp
from jax import lax
from jax.experimental import pallas as pl
from jax.experimental.pallas import tpu as pltpu
from jax.sharding import PartitionSpec as P

ITERS = 3
F32 = jnp.float32
BF16 = jnp.bfloat16
MESH = pl.DeviceIdType.MESH
SLOTS = 3
COARSE = 4


def adjoint_rows(src, co, low, count, emit):
    co_a, co_b, co_d = co
    cols = src.shape[-1]
    before = co_d[low - 1] * src[low - 1]
    y = src[low]
    here = co_d[low] * y
    for row in range(low, low + count):
        y_next = src[row + 1]
        after = co_d[row + 1] * y_next
        value = (
            co_a[row] * y
            + (before + after)
            + pltpu.roll(here, 1, 1)
            + pltpu.roll(co_b[row] * y, cols - 1, 1)
        )
        emit(row, value)
        before, here, y = here, after, y_next


def shift_groups(value, by):
    groups = value.shape[0]
    at = lax.broadcasted_iota(jnp.int32, value.shape, 0)
    outside = 0 if by == 1 else groups - 1
    return jnp.where(at == outside, 0.0, pltpu.roll(value, by % groups, 0))


def level_forward(src, dst, co):
    co_a, co_b, co_d = co
    rows, cols = src.shape[0], src.shape[-1]
    above = shift_groups(src[rows - 1], 1)
    here = first = src[0]
    for row in range(rows):
        below = src[row + 1] if row + 1 < rows else shift_groups(first, -1)
        dst[row] = (
            co_a[row] * here
            + co_d[row] * (above + below + pltpu.roll(here, cols - 1, 1))
            + co_b[row] * pltpu.roll(here, 1, 1)
        )
        above, here = here, below


def level_backward(src, dst, state, weight, co):
    co_a, co_b, co_d = co
    rows, cols = src.shape[0], src.shape[-1]
    above = shift_groups(co_d[rows - 1] * src[rows - 1], 1)
    y = src[0]
    here = first = co_d[0] * y
    for row in range(rows):
        y_next = src[row + 1] if row + 1 < rows else None
        below = shift_groups(first, -1) if y_next is None else co_d[row + 1] * y_next
        dst[row] = (
            co_a[row] * y
            + (above + below)
            + pltpu.roll(here, 1, 1)
            + pltpu.roll(co_b[row] * y, cols - 1, 1)
            + weight[row] * state[row]
        )
        above, here, y = here, below, y_next


def assimilate_kernel(
    n_space,
    n_tm,
    inn,
    obs,
    diff,
    cour,
    control,
    residual,
    inbuf,
    summed,
    turned,
    fields,
    counts,
    forcing,
    p_a,
    p_b,
    p_d,
    p_lam,
    p_send,
    p_recv,
    edge_src,
    edge_recv,
    halo_src,
    halo_recv,
    c_a,
    c_b,
    c_d,
    lam_0,
    lam_1,
    l_send,
    l_recv,
    f_recv,
    v_a,
    v_b,
    v_d,
    states,
    wts,
    adj_0,
    adj_1,
    resid,
    q_0,
    d_1,
    u_1,
    r_send,
    r_recv,
    red_src,
    red_recv,
    steps_ab,
    in_sems,
    loc_sems,
    w_send,
    w_recv,
    core_recv,
    edge_sems,
    halo_sems,
    f_sems,
    p_sems,
    l_sems,
    r_sems,
    red_sems,
):
    steps = forcing.shape[0]
    part, cols = forcing.shape[2:]
    rows = resid.shape[0]
    fine_rows = inbuf.shape[2]
    total = steps * n_tm
    halo = total - 1
    reach = steps - 1
    margin = reach + 1
    pad = halo + 1
    span = l_send.shape[1] // n_space
    pieces = cols // 128
    own_rows = steps * rows
    wide = 128 * COARSE
    n_z, n_x = n_space // 2, n_tm // 2
    place = lax.axis_index("space")
    section = lax.axis_index("tm")
    z, y = lax.div(place, 2), lax.rem(place, 2)
    x, core = lax.div(section, 2), lax.rem(section, 2)
    above, below = place - 1, place + 1
    has_above, has_below = place > 0, place < n_space - 1
    tm_peers = [lax.rem(section + k, n_tm) for k in range(1, n_tm)]
    space_peers = [lax.rem(place + k, n_space) for k in range(1, n_space)]
    everyone = [
        {"space": lax.rem(place + j, n_space), "tm": lax.rem(section + k, n_tm)}
        for j in range(n_space)
        for k in range(n_tm)
        if j or k
    ]
    lanes = [slice(piece * 128, (piece + 1) * 128) for piece in range(pieces)]

    def to(axis, peer):
        return {"device_id": {axis: peer}, "device_id_type": MESH}

    def remote(src, dst, send_sem, recv_sem, axis, peer):
        return pltpu.make_async_remote_copy(
            src_ref=src, dst_ref=dst, send_sem=send_sem, recv_sem=recv_sem, **to(axis, peer)
        )

    def slab(ref, index, size):
        return ref.at[:, pl.ds(pl.multiple_of(index * size, 8), size), :]

    def group_of(turn):
        d_x = lax.rem(lax.div(turn, 2) + 1, n_x)
        d_core = lax.rem(turn + 1, 2)
        return lax.rem(x + d_x, n_x) * 2 + lax.rem(core + d_core, 2)

    def block_copy(k):
        turn, t, slot = lax.div(k, steps), lax.rem(k, steps), lax.rem(k, SLOTS)
        return pltpu.make_async_copy(
            inn.at[t, pl.ds(group_of(turn) * part, part)], inbuf.at[slot], in_sems.at[slot]
        )

    own_counts = slab(counts.at[section], place, own_rows)
    local = []
    for piece in range(pieces):
        local.append(
            pltpu.make_async_copy(obs.at[:, lanes[piece]], own_counts.at[piece], loc_sems.at[piece, 0])
        )
        for k, field in enumerate((diff, cour)):
            local.append(
                pltpu.make_async_copy(
                    field.at[:, lanes[piece]], fields.at[k, piece], loc_sems.at[piece, 1 + k]
                )
            )
    for copy in local:
        copy.start()
    block_copy(jnp.int32(0)).start()

    edge_recv[...] = jnp.zeros_like(edge_recv)
    halo_recv[...] = jnp.zeros_like(halo_recv)
    barrier = pltpu.get_barrier_semaphore()
    for peer in everyone:
        pl.semaphore_signal(barrier, inc=1, device_id=peer, device_id_type=MESH)

    forcing[...] = jnp.zeros_like(forcing)
    p_lam[...] = jnp.zeros_like(p_lam)
    for ref in (p_a, p_b, p_d, c_a, c_b, c_d, lam_0, lam_1):
        ref[...] = jnp.zeros_like(ref)

    for copy in local:
        copy.wait()
    for k in range(1, SLOTS):
        block_copy(jnp.int32(k)).start()

    def by_level(k, group, row, piece):
        return fields[k, piece, pl.ds(group * (part * rows) + row, part, stride=rows), :]

    for k in range(2):
        for piece in range(pieces):
            at = lanes[piece]
            for side, row in enumerate((0, rows - 1)):
                for group in range(n_tm):
                    edge_src[k, side, group, :, at] = by_level(k, group, row, piece)
            for side, first in enumerate((0, rows - halo)):
                for row in range(halo):
                    halo_src[k, side, row, :, at] = by_level(k, section, first + row, piece)

    pl.semaphore_wait(barrier, len(everyone))

    def pair(src, dst, sems):
        up = remote(src.at[0], dst.at[1], sems.at[0, 0], sems.at[1, 0], "space", above)
        down = remote(src.at[1], dst.at[0], sems.at[0, 1], sems.at[1, 1], "space", below)
        return [(has_above, has_below, up), (has_below, has_above, down)]

    def start(copies):
        for sends, _, copy in copies:
            pl.when(sends)(copy.start)

    def finish(copies):
        for sends, receives, copy in copies:
            pl.when(sends)(copy.wait_send)
            pl.when(receives)(copy.wait_recv)

    edge_copies = pair_copies = []
    edge_copies = pair(edge_src.at[0], edge_recv.at[0], edge_sems.at[0])
    edge_copies += pair(edge_src.at[1], edge_recv.at[1], edge_sems.at[1])
    start(edge_copies)

    halo_copies = pair(halo_src.at[0], halo_recv.at[0], halo_sems.at[0])
    halo_copies += pair(halo_src.at[1], halo_recv.at[1], halo_sems.at[1])

    w_copies = []
    x_peers = [lax.rem(x + d_x, n_x) * 2 + core for d_x in range(1, n_x)]
    y_peer = z * 2 + (1 - y)

    def count_block(owner, owner_place):
        return slab(counts.at[owner], owner_place, own_rows)

    def count_send(owner, owner_place, axis, peer, valid=None):
        block = count_block(owner, owner_place)
        copy = remote(
            block, block, w_send.at[len(w_copies)], w_recv.at[owner, owner_place], axis, peer
        )
        if valid is None:
            copy.start()
        else:
            pl.when(valid)(copy.start)
        w_copies.append((valid, copy))

    def count_wait(owner, owner_place, valid=None):
        block = count_block(owner, owner_place)
        copy = remote(block, block, w_send.at[0], w_recv.at[owner, owner_place], "space", y_peer)
        if valid is None:
            copy.wait_recv()
        else:
            pl.when(valid)(copy.wait_recv)

    def inside_line(at):
        return jnp.logical_and(at >= 0, at < n_z)

    def count_pass(distance):
        for sign in (-1, 1) if distance else (0,):
            at = z + sign * distance
            valid = inside_line(at) if distance else None
            owner_place = at * 2 + y
            if distance:
                count_wait(section, owner_place, valid)
            for onward in (-sign,) if distance else (-1, 1):
                goes = inside_line(z + onward)
                if distance:
                    goes = jnp.logical_and(valid, goes)
                if distance < n_z - 1:
                    count_send(section, owner_place, "space", place + 2 * onward, goes)
            count_send(section, owner_place, "space", y_peer, valid)
            for peer in x_peers:
                count_send(section, owner_place, "tm", peer, valid)

    count_pass(0)

    f_copies = []

    def send_fields():
        for k in range(2):
            for j, peer in enumerate(space_peers):
                copy = remote(
                    slab(fields.at[k], section * part + peer, rows),
                    slab(f_recv.at[k], place, rows),
                    f_sems.at[k, 0, j],
                    f_sems.at[k, 1, place],
                    "space",
                    peer,
                )
                copy.start()
                f_copies.append(copy)
            slab(f_recv.at[k], place, rows)[...] = slab(
                fields.at[k], section * part + place, rows
            )[...]

    pick = jnp.where(
        lax.broadcasted_iota(jnp.int32, (wide, 128), 0) // COARSE
        == lax.broadcasted_iota(jnp.int32, (wide, 128), 1),
        1.0 / (COARSE * COARSE),
        0.0,
    ).astype(BF16)

    def restrict(turn, t):
        k = turn * steps + t
        block_copy(k).wait()
        slot = lax.rem(k, SLOTS)
        for piece in range(pieces):
            block = inbuf[slot, :, :, piece * wide : (piece + 1) * wide].reshape(part * fine_rows, wide)
            summed[piece] = jnp.dot(block, pick, preferred_element_type=F32)
        pl.when(k + SLOTS < total)(lambda: block_copy(k + SLOTS).start())
        for piece in range(pieces):
            first = pl.multiple_of(place * own_rows + t * rows, 8)
            scale = counts[section, piece, pl.ds(first, rows), :].astype(F32)
            for level in range(part):
                value = summed[piece, pl.ds(level * fine_rows, rows, stride=COARSE), :]
                for sub in range(1, COARSE):
                    value += summed[piece, pl.ds(level * fine_rows + sub, rows, stride=COARSE), :]
                turned[piece, pl.ds(level, rows, stride=part), :] = value * scale
            forcing[t, pl.ds(margin, rows), :, lanes[piece]] = turned[piece].reshape(rows, part, 128)

    def put(co, row, d, c, at=slice(None), inside=None):
        a = 1.0 - 4.0 * d - c
        if inside is not None:
            a = jnp.where(inside, a, 0.0)
        co[0][row, :, at] = a
        co[1][row, :, at] = d + c
        co[2][row, :, at] = d

    p_co = (p_a, p_b, p_d)
    reach_rows = rows + 2 * reach

    def carry_back(turn):
        group = group_of(turn)
        for row in range(rows):
            for piece in range(pieces):
                d, c = by_level(0, group, row, piece), by_level(1, group, row, piece)
                put(p_co, margin + row, d, c, lanes[piece])
        put(p_co, margin - 1, edge_recv[0, 0, group], edge_recv[1, 0, group], inside=has_above)
        put(p_co, margin + rows, edge_recv[0, 1, group], edge_recv[1, 1, group], inside=has_below)
        now = forcing.at[steps - 1]
        for k in range(1, steps):
            t = steps - 1 - k

            def emit(row, value, k=k, t=t):
                value = value + forcing[t, row]
                if k < steps - 1:
                    p_lam[k % 2, row] = value
                else:
                    p_send[turn, row - (margin - reach)] = value

            adjoint_rows(now, p_co, margin - reach, reach_rows, emit)
            now = p_lam.at[k % 2]

    def p_copy(turn):
        return remote(
            p_send.at[turn],
            p_recv.at[section],
            p_sems.at[0, turn],
            p_sems.at[1, section],
            "tm",
            group_of(turn),
        )

    def one_step(t, turn):
        restrict(turn, t)
        return turn

    for turn in range(n_tm):
        lax.fori_loop(0, steps, one_step, jnp.int32(turn))
        if turn == 0:
            finish(edge_copies)
            start(halo_copies)
        carry_back(jnp.int32(turn))
        if turn < n_tm - 1:
            p_copy(jnp.int32(turn)).start()
        for distance in range(1, n_z):
            if distance % n_tm == turn + 1:
                count_pass(distance)
        if turn == 1:
            send_fields()

    finish(halo_copies)
    c_co = (c_a, c_b, c_d)
    for row in range(rows):
        for piece in range(pieces):
            d, c = by_level(0, section, row, piece), by_level(1, section, row, piece)
            put(c_co, pad + row, d, c, lanes[piece])
    for row in range(halo):
        put(c_co, pad - halo + row, halo_recv[0, 0, row], halo_recv[1, 0, row], inside=has_above)
        put(c_co, pad + rows + row, halo_recv[0, 1, row], halo_recv[1, 1, row], inside=has_below)
    p_recv[section] = p_send[n_tm - 1]
    for k, peer in enumerate(tm_peers):
        p_copy(jnp.int32(k)).wait_send()
        remote(
            p_send.at[0], p_recv.at[peer], p_sems.at[0, 0], p_sems.at[1, peer], "tm", peer
        ).wait_recv()
    lam = [lam_0, lam_1]
    for row in range(reach_rows):
        lam_0[pad - reach + row] = p_recv[n_tm - 1, row]
    slot, grown = 0, reach
    for other in range(n_tm - 2, -1, -1):
        for k in range(steps):
            grown += 1
            last = other == 0 and k == steps - 1

            def emit(row, value, k=k, other=other, slot=slot, last=last):
                inside = row - (pad - reach)
                if k == steps - 1 and 0 <= inside < reach_rows:
                    value = value + p_recv[other, inside]
                if last:
                    for piece in range(pieces):
                        at = pl.ds(row - (pad - halo), part, stride=span)
                        l_send[piece, at, :] = value[:, lanes[piece]]
                else:
                    lam[1 - slot][row] = value

            adjoint_rows(lam[slot], c_co, pad - grown, rows + 2 * grown, emit)
            slot = 1 - slot

    l_copies = []
    for j, peer in enumerate(space_peers):
        copy = remote(
            slab(l_send, peer, span),
            slab(l_recv, place, span),
            l_sems.at[0, j],
            l_sems.at[1, place],
            "space",
            peer,
        )
        copy.start()
        l_copies.append(copy)
    slab(l_recv, place, span)[...] = slab(l_send, place, span)[...]

    line = [lax.rem(z + k, n_z) for k in range(n_z)]
    for at in line:
        owner_place = at * 2 + (1 - y)
        count_wait(section, owner_place)
        for peer in x_peers:
            count_send(section, owner_place, "tm", peer)
    for k in range(2):
        for peer in space_peers:
            block = slab(f_recv.at[k], peer, rows)
            remote(block, block, f_sems.at[k, 0, 0], f_sems.at[k, 1, peer], "space", peer).wait_recv()
    v_co = (v_a, v_b, v_d)
    for row in range(rows):
        for piece in range(pieces):
            at = pl.ds(row, n_space, stride=rows)
            put(v_co, row, f_recv[0, piece, at, :], f_recv[1, piece, at, :], lanes[piece])

    for at in line:
        for peer in x_peers:
            count_wait(peer, at * 2 + y)
            count_wait(peer, at * 2 + (1 - y))
    mine = [lax.rem(x + d_x, n_x) * 2 + core for d_x in range(n_x)]
    theirs = [lax.rem(x + d_x, n_x) * 2 + (1 - core) for d_x in range(n_x)]
    for owner in mine:
        block = counts.at[owner]
        copy = remote(
            block, block, w_send.at[len(w_copies)], core_recv.at[owner], "tm", x * 2 + (1 - core)
        )
        copy.start()
        w_copies.append((None, copy))

    def spread_counts(owner):
        def one(t, carry):
            for row in range(rows):
                for piece in range(pieces):
                    value = counts[owner, piece, pl.ds(t * rows + row, n_space, stride=own_rows), :]
                    wts[owner * steps + t, row, :, lanes[piece]] = value.astype(F32)
            return carry

        lax.fori_loop(0, steps, one, 0)

    for owner in mine:
        spread_counts(owner)
    for owner in theirs:
        block = counts.at[owner]
        remote(
            block, block, w_send.at[0], core_recv.at[owner], "tm", x * 2 + (1 - core)
        ).wait_recv()
        spread_counts(owner)

    for j, peer in enumerate(space_peers):
        block = slab(l_recv, peer, span)
        remote(block, block, l_sems.at[0, 0], l_sems.at[1, peer], "space", peer).wait_recv()

    def received(row, piece):
        return l_recv[piece, pl.ds(row, n_space, stride=span), :]

    for row in range(rows):
        for piece in range(pieces):
            value = received(halo + row, piece)
            from_below = row - (rows - halo)
            if from_below >= 0:
                value = value + shift_groups(received(from_below, piece), -1)
            if row < halo:
                value = value + shift_groups(received(halo + rows + row, piece), 1)
            resid[row, :, lanes[piece]] = value
            r_send[0, piece, pl.ds(row, n_space, stride=rows), :] = value

    def residual_copy(k, j, peer):
        return remote(
            slab(r_send.at[k], peer, rows),
            slab(r_recv.at[k], place, rows),
            r_sems.at[k, 0, j],
            r_sems.at[k, 1, place],
            "space",
            peer,
        )

    def send_residual(k):
        for j, peer in enumerate(space_peers):
            residual_copy(k, j, peer).start()
        slab(r_recv.at[k], place, rows)[...] = slab(r_send.at[k], place, rows)[...]

    def peer_slot(peer):
        return peer["tm"] * n_space + peer["space"]

    me = section * n_space + place

    def reduce_all(k, partials, meanwhile):
        at = lax.broadcasted_iota(jnp.int32, (16, 128), 0)
        lane = lax.broadcasted_iota(jnp.int32, (16, 128), 1)
        tile = jnp.zeros((16, 128), F32)
        for j, partial in enumerate(partials):
            folded = partial[:, lanes[0]]
            for piece in range(1, pieces):
                folded = folded + partial[:, lanes[piece]]
            tile = jnp.where(at == j, jnp.sum(folded, axis=0, keepdims=True), tile)
        tile = jnp.where(at == lane, jnp.sum(tile, axis=1, keepdims=True), 0.0)
        line = jnp.sum(tile, axis=0, keepdims=True)
        red_src[k] = line
        red_recv[k, me] = line
        copies = [
            pltpu.make_async_remote_copy(
                src_ref=red_src.at[k],
                dst_ref=red_recv.at[k, me],
                send_sem=red_sems.at[k, 0, j],
                recv_sem=red_sems.at[k, 1, me],
                device_id=peer,
                device_id_type=MESH,
            )
            for j, peer in enumerate(everyone)
        ]
        for copy in copies:
            copy.start()
        meanwhile()
        for j, peer in enumerate(everyone):
            copies[j].wait_send()
            pltpu.make_async_remote_copy(
                src_ref=red_src.at[k],
                dst_ref=red_recv.at[k, peer_slot(peer)],
                send_sem=red_sems.at[k, 0, j],
                recv_sem=red_sems.at[k, 1, peer_slot(peer)],
                device_id=peer,
                device_id_type=MESH,
            ).wait_recv()
        line = red_recv[k, 0]
        for j in range(1, n_tm * n_space):
            line = line + red_recv[k, j]
        line = jnp.broadcast_to(line, (8, 128))
        lane = lane[:8]
        return [
            jnp.sum(jnp.where(lane == j, line, 0.0), axis=1, keepdims=True)[0:1]
            for j in range(len(partials))
        ]

    adj = [adj_0, adj_1]
    image = adj[(total - 1) % 2]

    def keep_residual(k, row, value):
        for piece in range(pieces):
            r_send[k, piece, pl.ds(row, n_space, stride=rows), :] = value[:, lanes[piece]]

    def scalar(k):
        return steps_ab[k, 0:1, 0:1]

    def set_scalar(k, value):
        steps_ab[k] = jnp.broadcast_to(value, (8, 128))

    def dots(names, vectors):
        sums = [jnp.zeros((n_space, cols), F32)] * len(names)
        for row in range(rows):
            at = vectors(row)
            sums = [total_ + at[pair_[0]] * at[pair_[1]] for total_, pair_ in zip(sums, names)]
        return sums

    def first_step():
        def vectors(row):
            r = resid[row]
            q = r + image[row]
            q_0[row] = q
            return {"r": r, "q": q}

        rr, rq, qq = reduce_all(0, dots(("rr", "rq", "qq"), vectors), lambda: send_residual(0))
        alpha = rr / rq
        beta = (rr - 2.0 * alpha * rq + alpha * alpha * qq) / rr
        set_scalar(0, alpha)
        set_scalar(1, beta)
        for row in range(rows):
            r_0 = resid[row]
            r = r_0 - alpha * q_0[row]
            resid[row] = r
            keep_residual(1, row, r)
            d = r + beta * r_0
            d_1[row] = d
            states[0, row] = d
        send_residual(1)

    def second_image():
        for row in range(rows):
            u = states[0, row] + image[row]
            u_1[row] = u
            states[0, row] = u
            keep_residual(2, row, u)

    def last_steps():
        def vectors(row):
            u = u_1[row]
            v = u + image[row]
            image[row] = v
            return {"r": resid[row], "d": d_1[row], "u": u, "v": v, "q": q_0[row]}

        names = ("rr", "du", "ru", "uu", "rq", "uq", "dq", "rv", "uv", "dv")
        rr, du, ru, uu, rq, uq, dq, rv, uv, dv = reduce_all(
            1, dots(names, vectors), lambda: send_residual(2)
        )
        beta_1 = scalar(1)
        alpha = rr / du
        rr_2 = rr - 2.0 * alpha * ru + alpha * alpha * uu
        beta = rr_2 / rr
        on_u, on_q, on_v = 1.0 + beta, -beta_1, -alpha
        curve = (
            (on_u * ru + on_q * rq + on_v * rv)
            - alpha * (on_u * uu + on_q * uq + on_v * uv)
            + beta * (on_u * du + on_q * dq + on_v * dv)
        )
        alpha_2 = rr_2 / curve
        for row in range(rows):
            u = u_1[row]
            r_2 = resid[row] - alpha * u
            keep_residual(3, row, r_2 - alpha_2 * (on_u * u + on_q * q_0[row] + on_v * image[row]))
        send_residual(3)
        kept = alpha + alpha_2 * beta
        set_scalar(2, scalar(0) + kept * beta_1)
        set_scalar(3, kept + alpha_2)
        set_scalar(4, -alpha * alpha_2)

    def one_product(k, carry):
        for t in range(1, total):
            level_forward(states.at[t - 1], states.at[t], v_co)
        for row in range(rows):
            adj_0[row] = wts[total - 1, row] * states[total - 1, row]
        slot = 0
        for t in range(total - 2, -1, -1):
            level_backward(adj[slot], adj[1 - slot], states.at[t], wts.at[t], v_co)
            slot = 1 - slot
        pl.when(k == 0)(first_step)
        pl.when(k == 1)(second_image)
        pl.when(k == 2)(last_steps)
        return carry

    states[0] = resid[...]
    lax.fori_loop(0, ITERS, one_product, 0)

    def residual_arrived(k):
        for peer in space_peers:
            block = slab(r_recv.at[k], peer, rows)
            remote(block, block, r_sems.at[k, 0, 0], r_sems.at[k, 1, peer], "space", peer).wait_recv()

    for k in range(ITERS):
        residual_arrived(k)
    for piece in range(pieces):
        value = steps_ab[2, 0:1, :] * r_recv[0, piece]
        for k in range(1, ITERS):
            value = value + steps_ab[2 + k, 0:1, :] * r_recv[k, piece]
        control[piece] = value
    residual_arrived(ITERS)
    residual[...] = r_recv[ITERS]

    for k in range(ITERS + 1):
        for j, peer in enumerate(space_peers):
            residual_copy(k, j, peer).wait_send()
    for valid, copy in w_copies:
        if valid is None:
            copy.wait_send()
        else:
            pl.when(valid)(copy.wait_send)
    for copy in f_copies + l_copies:
        copy.wait_send()


def assimilate_call(innovations, obs_counts, diffusion, courant, n_space, n_tm):
    steps, levels, fine_rows, fine_cols = innovations.shape
    part = levels // n_tm
    rows, cols = fine_rows // COARSE, fine_cols // COARSE
    pieces = cols // 128
    total = steps * n_tm
    halo = total - 1
    reach = steps - 1
    padded = rows + 2 * (reach + 1)
    ext = rows + 2 * (halo + 1)
    span = -(-(rows + 2 * halo) // 8) * 8
    row = (part, cols)
    n_x, n_z = n_tm // 2, n_space // 2
    sends = 2 + n_x + 2 * (n_z - 1) * (1 + n_x) + n_z * (n_x - 1) + n_x
    dma = pltpu.SemaphoreType.DMA
    shapes = [
        pltpu.VMEM((SLOTS, part, fine_rows, fine_cols), BF16),
        pltpu.VMEM((pieces, part * fine_rows, 128), F32),
        pltpu.VMEM((pieces, part * rows, 128), F32),
        pltpu.VMEM((2, pieces, levels * rows, 128), F32),
        pltpu.VMEM((n_tm, pieces, n_space * steps * rows, 128), jnp.int32),
        pltpu.VMEM((steps, padded, *row), F32),
        pltpu.VMEM((padded, *row), F32),
        pltpu.VMEM((padded, *row), F32),
        pltpu.VMEM((padded, *row), F32),
        pltpu.VMEM((2, padded, *row), F32),
        pltpu.VMEM((n_tm, rows + 2 * reach, *row), F32),
        pltpu.VMEM((n_tm, rows + 2 * reach, *row), F32),
        pltpu.VMEM((2, 2, n_tm, *row), F32),
        pltpu.VMEM((2, 2, n_tm, *row), F32),
        pltpu.VMEM((2, 2, halo, *row), F32),
        pltpu.VMEM((2, 2, halo, *row), F32),
        pltpu.VMEM((ext, *row), F32),
        pltpu.VMEM((ext, *row), F32),
        pltpu.VMEM((ext, *row), F32),
        pltpu.VMEM((ext, *row), F32),
        pltpu.VMEM((ext, *row), F32),
        pltpu.VMEM((pieces, n_space * span, 128), F32),
        pltpu.VMEM((pieces, n_space * span, 128), F32),
        pltpu.VMEM((2, pieces, n_space * rows, 128), F32),
        pltpu.VMEM((rows, n_space, cols), F32),
        pltpu.VMEM((rows, n_space, cols), F32),
        pltpu.VMEM((rows, n_space, cols), F32),
        pltpu.VMEM((total, rows, n_space, cols), F32),
        pltpu.VMEM((total, rows, n_space, cols), F32),
        pltpu.VMEM((rows, n_space, cols), F32),
        pltpu.VMEM((rows, n_space, cols), F32),
        pltpu.VMEM((rows, n_space, cols), F32),
        pltpu.VMEM((rows, n_space, cols), F32),
        pltpu.VMEM((rows, n_space, cols), F32),
        pltpu.VMEM((rows, n_space, cols), F32),
        pltpu.VMEM((ITERS + 1, pieces, n_space * rows, 128), F32),
        pltpu.VMEM((ITERS + 1, pieces, n_space * rows, 128), F32),
        pltpu.VMEM((2, 1, 128), F32),
        pltpu.VMEM((2, n_tm * n_space, 1, 128), F32),
        pltpu.VMEM((5, 8, 128), F32),
        dma((SLOTS,)),
        dma((pieces, 3)),
        dma((sends,)),
        dma((n_tm, n_space)),
        dma((n_tm,)),
        dma((2, 2, 2)),
        dma((2, 2, 2)),
        dma((2, 2, n_space)),
        dma((2, n_tm)),
        dma((2, n_space)),
        dma((ITERS + 1, 2, n_space)),
        dma((2, 2, n_tm * n_space)),
    ]
    out = jax.ShapeDtypeStruct((pieces, part * rows, 128), F32)
    return pl.pallas_call(
        functools.partial(assimilate_kernel, n_space, n_tm),
        out_shape=[out] * 2,
        in_specs=[pl.BlockSpec(memory_space=pl.ANY)] * 4,
        out_specs=[pl.BlockSpec(memory_space=pltpu.VMEM)] * 2,
        scratch_shapes=shapes,
        compiler_params=pltpu.CompilerParams(
            collective_id=0, has_side_effects=True, vmem_limit_bytes=60 * 2**20
        ),
        name="assimilate",
    )(
        innovations,
        obs_counts.reshape(steps * rows, cols),
        diffusion.reshape(levels * rows, cols),
        courant.reshape(levels * rows, cols),
    )


def expand_kernel(control, residual, increment, residual_out, held, passed, repeated, wide_out, in_sems, out_sems):
    pieces, part, rows, _ = control.shape
    wide = 128 * COARSE
    arrive = []
    for k, (src, dst) in enumerate(((control, held), (residual, passed))):
        arrive.append(pltpu.make_async_copy(src, dst, in_sems.at[k]))
        arrive[k].start()
    pick = jnp.where(
        lax.broadcasted_iota(jnp.int32, (256, wide), 1) // COARSE
        == lax.rem(lax.broadcasted_iota(jnp.int32, (256, wide), 0), 128),
        1.0,
        0.0,
    ).astype(BF16)
    leave = []
    arrive[0].wait()
    for level in range(part):
        for piece in range(pieces):
            values = held[piece, level]
            for sub in range(COARSE):
                repeated[level % 2, piece, pl.ds(sub, rows, stride=COARSE), :] = values
            whole = repeated[level % 2, piece]
            head = whole.astype(BF16)
            rest = (whole - head.astype(F32)).astype(BF16)
            both = jnp.concatenate([head, rest], axis=1)
            wide_out[level, :, piece * wide : (piece + 1) * wide] = jnp.dot(
                both, pick, preferred_element_type=F32
            )
        leave.append(
            pltpu.make_async_copy(wide_out.at[level], increment.at[level], out_sems.at[level])
        )
        leave[-1].start()
        if level == 0:
            arrive[1].wait()
            for piece in range(pieces):
                at = pl.ds(piece * 128, 128)
                leave.append(
                    pltpu.make_async_copy(
                        passed.at[piece], residual_out.at[:, :, at], out_sems.at[part + piece]
                    )
                )
                leave[-1].start()
    for copy in leave:
        copy.wait()


def expand_call(control, residual, part):
    pieces, count, _ = control.shape
    rows, cols = count // part, pieces * 128
    fine = (part, rows * COARSE, cols * COARSE)
    cut = (pieces, part, rows, 128)
    dma = pltpu.SemaphoreType.DMA
    return pl.pallas_call(
        expand_kernel,
        in_specs=[pl.BlockSpec(memory_space=pl.ANY)] * 2,
        out_specs=[pl.BlockSpec(memory_space=pl.ANY)] * 2,
        out_shape=[
            jax.ShapeDtypeStruct(fine, F32),
            jax.ShapeDtypeStruct((part, rows, cols), F32),
        ],
        scratch_shapes=[
            pltpu.VMEM(cut, F32),
            pltpu.VMEM(cut, F32),
            pltpu.VMEM((2, pieces, rows * COARSE, 128), F32),
            pltpu.VMEM(fine, F32),
            dma((2,)),
            dma((part + pieces,)),
        ],
        compiler_params=pltpu.CompilerParams(vmem_limit_bytes=67_043_328),
        name="expand",
    )(control.reshape(cut), residual.reshape(cut))


def padded_2(cells, sides, width):
    for axis, dim in sides:
        count = lax.axis_size(axis)
        ends = count - 1
        head = lax.slice_in_dim(cells, 0, width, axis=dim)
        tail = lax.slice_in_dim(cells, cells.shape[dim] - width, cells.shape[dim], axis=dim)
        cells = jnp.concatenate(
            [
                lax.ppermute(tail, axis, [(i, (i + 1) % count) for i in range(ends)]),
                cells,
                lax.ppermute(head, axis, [((i + 1) % count, i) for i in range(ends)]),
            ],
            axis=dim,
        )
    return cells


def laplace_rows(padded, state_field):
    return (
        padded[:, 2:, :]
        + padded[:, :-2, :]
        + jnp.roll(state_field, 1, 2)
        + jnp.roll(state_field, -1, 2)
        - 4.0 * state_field
    )


def tangent(state_field, diffusion, courant):
    padded = padded_2(state_field, (("space", 1),), 1)
    return (
        state_field
        + diffusion * laplace_rows(padded, state_field)
        - courant * (state_field - jnp.roll(state_field, 1, 2))
    )


def adjoint(state_field, diffusion, courant):
    carried = courant * state_field
    spread = diffusion * state_field
    padded = padded_2(spread, (("space", 1),), 1)
    return state_field + laplace_rows(padded, spread) - carried + jnp.roll(carried, -1, 2)


def level_squares(residual):
    return lax.psum(jnp.sum(residual * residual), ("space", "tm"))


def level_curve(direction, hessian_image):
    return lax.psum(jnp.sum(direction * hessian_image), ("space", "tm"))


def solve_inner(rhs_field, hessian_part, norm_fn, curve_fn):
    control = jnp.zeros_like(rhs_field)
    residual = rhs_field
    direction = rhs_field
    norm_now = norm_fn(residual)
    for iter_no in range(ITERS):
        hessian_image = direction + hessian_part(direction)
        step_len = norm_now / curve_fn(direction, hessian_image)
        control = control + step_len * direction
        residual = residual - step_len * hessian_image
        if iter_no + 1 < ITERS:
            norm_next = norm_fn(residual)
            direction = residual + norm_next / norm_now * direction
            norm_now = norm_next
    return (control, residual)


def on_device(innovations, obs_counts, diffusion, courant):
    step_dev = obs_counts.shape[0]
    n_sections = lax.axis_size("tm")
    section_pos = lax.axis_index("tm")
    total_steps = step_dev * n_sections
    weights = obs_counts.astype(jnp.float32)[:, None]
    levels, fine_rows, fine_cols = (
        innovations.shape[1],
        innovations.shape[2],
        innovations.shape[3],
    )
    lev_part = levels // n_sections
    rows, cols = fine_rows // COARSE, fine_cols // COARSE
    n_space = lax.axis_size("space")
    tiled = lev_part == 8 and rows % 8 == 0 and cols % 128 == 0
    paired = n_space == lev_part and n_sections % 2 == 0
    if tiled and paired and rows >= total_steps - 1:
        solved = assimilate_call(innovations, obs_counts, diffusion, courant, n_space, n_sections)
        return tuple(expand_call(*solved, lev_part))
    blocks = innovations.reshape(step_dev, levels, fine_rows // 4, 4, fine_cols // 4, 4).astype(
        jnp.float32
    )
    forcing = weights * jnp.mean(blocks, axis=(3, 5))
    all_weights = lax.all_gather(obs_counts, "tm", axis=0, tiled=True).astype(jnp.float32)[:, None]
    all_forcing = lax.all_to_all(forcing, "tm", split_axis=1, concat_axis=0, tiled=True)
    diff_part = lax.dynamic_slice_in_dim(diffusion, section_pos * lev_part, lev_part, 0)
    cour_part = lax.dynamic_slice_in_dim(courant, section_pos * lev_part, lev_part, 0)

    def level_back(terms):
        current = terms[total_steps - 1]
        for step_no in range(total_steps - 2, -1, -1):
            current = terms[step_no] + adjoint(current, diff_part, cour_part)
        return current

    def level_hess(state_field):
        records = []
        for step_no in range(total_steps):
            records.append(all_weights[step_no] * state_field)
            if step_no + 1 < total_steps:
                state_field = tangent(state_field, diff_part, cour_part)
        return level_back(jnp.stack(records))

    control, residual = solve_inner(level_back(all_forcing), level_hess, level_squares, level_curve)
    increment = jnp.repeat(jnp.repeat(control, 4, axis=1), 4, axis=2)
    return (increment, residual)


def solution(mesh):
    placed = (
        P("tm", None, "space", None),
        P("tm", "space", None),
        P(None, "space", None),
        P(None, "space", None),
    )
    return jax.shard_map(
        on_device,
        mesh=mesh,
        in_specs=placed,
        out_specs=(P("tm", "space", None), P("tm", "space", None)),
        check_vma=False,
    )
```

```python
import functools

import jax
import jax.numpy as jnp
from jax import lax
from jax.experimental import pallas as pl
from jax.experimental.pallas import tpu as pltpu
from jax.sharding import PartitionSpec as P

ITERS = 3
F32 = jnp.float32
BF16 = jnp.bfloat16
MESH = pl.DeviceIdType.MESH
SLOTS = 3
COARSE = 4


def adjoint_rows(src, co, low, count, emit):
    co_a, co_b, co_d = co
    cols = src.shape[-1]
    before = co_d[low - 1] * src[low - 1]
    y = src[low]
    here = co_d[low] * y
    for row in range(low, low + count):
        y_next = src[row + 1]
        after = co_d[row + 1] * y_next
        value = (
            co_a[row] * y
            + (before + after)
            + pltpu.roll(here, 1, 1)
            + pltpu.roll(co_b[row] * y, cols - 1, 1)
        )
        emit(row, value)
        before, here, y = here, after, y_next


def shift_groups(value, by):
    groups = value.shape[0]
    at = lax.broadcasted_iota(jnp.int32, value.shape, 0)
    outside = 0 if by == 1 else groups - 1
    return jnp.where(at == outside, 0.0, pltpu.roll(value, by % groups, 0))


def level_forward(src, dst, co):
    co_a, co_b, co_d = co
    rows, cols = src.shape[0], src.shape[-1]
    above = shift_groups(src[rows - 1], 1)
    here = first = src[0]
    for row in range(rows):
        below = src[row + 1] if row + 1 < rows else shift_groups(first, -1)
        dst[row] = (
            co_a[row] * here
            + co_d[row] * (above + below + pltpu.roll(here, cols - 1, 1))
            + co_b[row] * pltpu.roll(here, 1, 1)
        )
        above, here = here, below


def level_backward(src, dst, state, weight, co):
    co_a, co_b, co_d = co
    rows, cols = src.shape[0], src.shape[-1]
    above = shift_groups(co_d[rows - 1] * src[rows - 1], 1)
    y = src[0]
    here = first = co_d[0] * y
    for row in range(rows):
        y_next = src[row + 1] if row + 1 < rows else None
        below = shift_groups(first, -1) if y_next is None else co_d[row + 1] * y_next
        dst[row] = (
            co_a[row] * y
            + (above + below)
            + pltpu.roll(here, 1, 1)
            + pltpu.roll(co_b[row] * y, cols - 1, 1)
            + weight[row] * state[row]
        )
        above, here, y = here, below, y_next


def assimilate_kernel(
    n_space,
    n_tm,
    inn,
    obs,
    diff,
    cour,
    control,
    residual,
    inbuf,
    summed,
    turned,
    fields,
    counts,
    forcing,
    p_a,
    p_b,
    p_d,
    p_lam,
    p_send,
    p_recv,
    edge_src,
    edge_recv,
    halo_src,
    halo_recv,
    c_a,
    c_b,
    c_d,
    lam_0,
    lam_1,
    l_send,
    l_recv,
    f_recv,
    v_a,
    v_b,
    v_d,
    states,
    wts,
    adj_0,
    adj_1,
    resid,
    q_0,
    d_1,
    u_1,
    r_send,
    r_recv,
    red_src,
    red_recv,
    steps_ab,
    in_sems,
    loc_sems,
    w_send,
    w_recv,
    core_recv,
    edge_sems,
    halo_sems,
    f_sems,
    p_sems,
    l_sems,
    r_sems,
    red_sems,
):
    steps = forcing.shape[0]
    part, cols = forcing.shape[2:]
    rows = resid.shape[0]
    fine_rows = inbuf.shape[2]
    total = steps * n_tm
    halo = total - 1
    apron = halo - 1
    reach = steps - 1
    margin = reach + 1
    pad = halo + 1
    span = l_send.shape[1] // n_space
    pieces = cols // 128
    own_rows = steps * rows
    wide = 128 * COARSE
    n_z, n_x = n_space // 2, n_tm // 2
    place = lax.axis_index("space")
    section = lax.axis_index("tm")
    z, y = lax.div(place, 2), lax.rem(place, 2)
    x, core = lax.div(section, 2), lax.rem(section, 2)
    above, below = place - 1, place + 1
    has_above, has_below = place > 0, place < n_space - 1
    tm_peers = [lax.rem(section + k, n_tm) for k in range(1, n_tm)]
    space_peers = [lax.rem(place + k, n_space) for k in range(1, n_space)]
    everyone = [
        {"space": lax.rem(place + j, n_space), "tm": lax.rem(section + k, n_tm)}
        for j in range(n_space)
        for k in range(n_tm)
        if j or k
    ]
    lanes = [slice(piece * 128, (piece + 1) * 128) for piece in range(pieces)]

    def to(axis, peer):
        return {"device_id": {axis: peer}, "device_id_type": MESH}

    def remote(src, dst, send_sem, recv_sem, axis, peer):
        return pltpu.make_async_remote_copy(
            src_ref=src, dst_ref=dst, send_sem=send_sem, recv_sem=recv_sem, **to(axis, peer)
        )

    def slab(ref, index, size):
        return ref.at[:, pl.ds(pl.multiple_of(index * size, 8), size), :]

    def group_of(turn):
        d_x = lax.rem(lax.div(turn, 2) + 1, n_x)
        d_core = lax.rem(turn + 1, 2)
        return lax.rem(x + d_x, n_x) * 2 + lax.rem(core + d_core, 2)

    def block_copy(k):
        turn, t, slot = lax.div(k, steps), lax.rem(k, steps), lax.rem(k, SLOTS)
        return pltpu.make_async_copy(
            inn.at[t, pl.ds(group_of(turn) * part, part)], inbuf.at[slot], in_sems.at[slot]
        )

    own_counts = slab(counts.at[section], place, own_rows)
    local = []
    for piece in range(pieces):
        local.append(
            pltpu.make_async_copy(obs.at[:, lanes[piece]], own_counts.at[piece], loc_sems.at[piece, 0])
        )
        for k, field in enumerate((diff, cour)):
            local.append(
                pltpu.make_async_copy(
                    field.at[:, lanes[piece]], fields.at[k, piece], loc_sems.at[piece, 1 + k]
                )
            )
    for copy in local:
        copy.start()
    block_copy(jnp.int32(0)).start()

    edge_recv[...] = jnp.zeros_like(edge_recv)
    halo_recv[...] = jnp.zeros_like(halo_recv)
    barrier = pltpu.get_barrier_semaphore()
    for peer in everyone:
        pl.semaphore_signal(barrier, inc=1, device_id=peer, device_id_type=MESH)

    forcing[...] = jnp.zeros_like(forcing)
    p_lam[...] = jnp.zeros_like(p_lam)
    for ref in (p_a, p_b, p_d, c_a, c_b, c_d, lam_0, lam_1):
        ref[...] = jnp.zeros_like(ref)

    for copy in local:
        copy.wait()
    for k in range(1, SLOTS):
        block_copy(jnp.int32(k)).start()

    def by_level(k, group, row, piece):
        return fields[k, piece, pl.ds(group * (part * rows) + row, part, stride=rows), :]

    for k in range(2):
        for piece in range(pieces):
            at = lanes[piece]
            for side, row in enumerate((0, rows - 1)):
                for group in range(n_tm):
                    edge_src[k, side, group, :, at] = by_level(k, group, row, piece)
            for side, first in enumerate((0, rows - apron)):
                for row in range(apron):
                    halo_src[k, side, row, :, at] = by_level(k, section, first + row, piece)

    pl.semaphore_wait(barrier, len(everyone))

    def pair(src, dst, sems):
        up = remote(src.at[0], dst.at[1], sems.at[0, 0], sems.at[1, 0], "space", above)
        down = remote(src.at[1], dst.at[0], sems.at[0, 1], sems.at[1, 1], "space", below)
        return [(has_above, has_below, up), (has_below, has_above, down)]

    def start(copies):
        for sends, _, copy in copies:
            pl.when(sends)(copy.start)

    def finish(copies):
        for sends, receives, copy in copies:
            pl.when(sends)(copy.wait_send)
            pl.when(receives)(copy.wait_recv)

    edge_copies = pair_copies = []
    edge_copies = pair(edge_src.at[0], edge_recv.at[0], edge_sems.at[0])
    edge_copies += pair(edge_src.at[1], edge_recv.at[1], edge_sems.at[1])
    start(edge_copies)

    halo_copies = pair(halo_src.at[0], halo_recv.at[0], halo_sems.at[0])
    halo_copies += pair(halo_src.at[1], halo_recv.at[1], halo_sems.at[1])

    w_copies = []
    x_peers = [lax.rem(x + d_x, n_x) * 2 + core for d_x in range(1, n_x)]
    y_peer = z * 2 + (1 - y)

    def count_block(owner, owner_place):
        return slab(counts.at[owner], owner_place, own_rows)

    def count_send(owner, owner_place, axis, peer, valid=None):
        block = count_block(owner, owner_place)
        copy = remote(
            block, block, w_send.at[len(w_copies)], w_recv.at[owner, owner_place], axis, peer
        )
        if valid is None:
            copy.start()
        else:
            pl.when(valid)(copy.start)
        w_copies.append((valid, copy))

    def count_wait(owner, owner_place, valid=None):
        block = count_block(owner, owner_place)
        copy = remote(block, block, w_send.at[0], w_recv.at[owner, owner_place], "space", y_peer)
        if valid is None:
            copy.wait_recv()
        else:
            pl.when(valid)(copy.wait_recv)

    def inside_line(at):
        return jnp.logical_and(at >= 0, at < n_z)

    def count_pass(distance):
        for sign in (-1, 1) if distance else (0,):
            at = z + sign * distance
            valid = inside_line(at) if distance else None
            owner_place = at * 2 + y
            if distance:
                count_wait(section, owner_place, valid)
            for onward in (-sign,) if distance else (-1, 1):
                goes = inside_line(z + onward)
                if distance:
                    goes = jnp.logical_and(valid, goes)
                if distance < n_z - 1:
                    count_send(section, owner_place, "space", place + 2 * onward, goes)
            count_send(section, owner_place, "space", y_peer, valid)
            for peer in x_peers:
                count_send(section, owner_place, "tm", peer, valid)

    count_pass(0)

    f_copies = []

    def send_fields():
        for k in range(2):
            for j, peer in enumerate(space_peers):
                copy = remote(
                    slab(fields.at[k], section * part + peer, rows),
                    slab(f_recv.at[k], place, rows),
                    f_sems.at[k, 0, j],
                    f_sems.at[k, 1, place],
                    "space",
                    peer,
                )
                copy.start()
                f_copies.append(copy)
            slab(f_recv.at[k], place, rows)[...] = slab(
                fields.at[k], section * part + place, rows
            )[...]

    pick = jnp.where(
        lax.broadcasted_iota(jnp.int32, (wide, 128), 0) // COARSE
        == lax.broadcasted_iota(jnp.int32, (wide, 128), 1),
        1.0 / (COARSE * COARSE),
        0.0,
    ).astype(BF16)

    def restrict(turn, t):
        k = turn * steps + t
        block_copy(k).wait()
        slot = lax.rem(k, SLOTS)
        for piece in range(pieces):
            block = inbuf[slot, :, :, piece * wide : (piece + 1) * wide].reshape(part * fine_rows, wide)
            summed[piece] = jnp.dot(block, pick, preferred_element_type=F32)
        pl.when(k + SLOTS < total)(lambda: block_copy(k + SLOTS).start())
        for piece in range(pieces):
            first = pl.multiple_of(place * own_rows + t * rows, 8)
            scale = counts[section, piece, pl.ds(first, rows), :].astype(F32)
            for level in range(part):
                value = summed[piece, pl.ds(level * fine_rows, rows, stride=COARSE), :]
                for sub in range(1, COARSE):
                    value += summed[piece, pl.ds(level * fine_rows + sub, rows, stride=COARSE), :]
                turned[piece, pl.ds(level, rows, stride=part), :] = value * scale
            forcing[t, pl.ds(margin, rows), :, lanes[piece]] = turned[piece].reshape(rows, part, 128)

    def put(co, row, d, c, at=slice(None), inside=None):
        a = 1.0 - 4.0 * d - c
        if inside is not None:
            a = jnp.where(inside, a, 0.0)
        co[0][row, :, at] = a
        co[1][row, :, at] = d + c
        co[2][row, :, at] = d

    p_co = (p_a, p_b, p_d)
    reach_rows = rows + 2 * reach

    def carry_back(turn):
        group = group_of(turn)
        for row in range(rows):
            for piece in range(pieces):
                d, c = by_level(0, group, row, piece), by_level(1, group, row, piece)
                put(p_co, margin + row, d, c, lanes[piece])
        put(p_co, margin - 1, edge_recv[0, 0, group], edge_recv[1, 0, group], inside=has_above)
        put(p_co, margin + rows, edge_recv[0, 1, group], edge_recv[1, 1, group], inside=has_below)
        now = forcing.at[steps - 1]
        for k in range(1, steps):
            t = steps - 1 - k

            def emit(row, value, k=k, t=t):
                value = value + forcing[t, row]
                if k < steps - 1:
                    p_lam[k % 2, row] = value
                else:
                    p_send[turn, row - (margin - reach)] = value

            adjoint_rows(now, p_co, margin - reach, reach_rows, emit)
            now = p_lam.at[k % 2]

    def p_copy(turn):
        return remote(
            p_send.at[turn],
            p_recv.at[section],
            p_sems.at[0, turn],
            p_sems.at[1, section],
            "tm",
            group_of(turn),
        )

    def one_step(t, turn):
        restrict(turn, t)
        return turn

    for turn in range(n_tm):
        lax.fori_loop(0, steps, one_step, jnp.int32(turn))
        if turn == 0:
            finish(edge_copies)
            start(halo_copies)
        carry_back(jnp.int32(turn))
        if turn < n_tm - 1:
            p_copy(jnp.int32(turn)).start()
        for distance in range(1, n_z):
            if distance % n_tm == turn:
                count_pass(distance)
        if turn == 1:
            send_fields()

    finish(halo_copies)
    c_co = (c_a, c_b, c_d)
    for row in range(rows):
        for piece in range(pieces):
            d, c = by_level(0, section, row, piece), by_level(1, section, row, piece)
            put(c_co, pad + row, d, c, lanes[piece])
    for row in range(apron):
        put(c_co, pad - apron + row, halo_recv[0, 0, row], halo_recv[1, 0, row], inside=has_above)
        put(c_co, pad + rows + row, halo_recv[0, 1, row], halo_recv[1, 1, row], inside=has_below)
    p_recv[section] = p_send[n_tm - 1]
    for k, peer in enumerate(tm_peers):
        p_copy(jnp.int32(k)).wait_send()
        remote(
            p_send.at[0], p_recv.at[peer], p_sems.at[0, 0], p_sems.at[1, peer], "tm", peer
        ).wait_recv()
    lam = [lam_0, lam_1]
    for row in range(reach_rows):
        lam_0[pad - reach + row] = p_recv[n_tm - 1, row]
    slot, grown = 0, reach
    for other in range(n_tm - 2, -1, -1):
        for k in range(steps):
            grown += 1
            last = other == 0 and k == steps - 1

            def emit(row, value, k=k, other=other, slot=slot, last=last):
                inside = row - (pad - reach)
                if k == steps - 1 and 0 <= inside < reach_rows:
                    value = value + p_recv[other, inside]
                if last:
                    for piece in range(pieces):
                        at = pl.ds(row - (pad - halo), part, stride=span)
                        l_send[piece, at, :] = value[:, lanes[piece]]
                else:
                    lam[1 - slot][row] = value

            adjoint_rows(lam[slot], c_co, pad - grown, rows + 2 * grown, emit)
            slot = 1 - slot

    l_copies = []
    for j, peer in enumerate(space_peers):
        copy = remote(
            slab(l_send, peer, span),
            slab(l_recv, place, span),
            l_sems.at[0, j],
            l_sems.at[1, place],
            "space",
            peer,
        )
        copy.start()
        l_copies.append(copy)
    slab(l_recv, place, span)[...] = slab(l_send, place, span)[...]

    line = [lax.rem(z + k, n_z) for k in range(n_z)]
    for at in line:
        owner_place = at * 2 + (1 - y)
        count_wait(section, owner_place)
        for peer in x_peers:
            count_send(section, owner_place, "tm", peer)
    core_peer = x * 2 + (1 - core)

    def core_send(owner):
        block = counts.at[owner]
        copy = remote(
            block, block, w_send.at[len(w_copies)], core_recv.at[owner], "tm", core_peer
        )
        copy.start()
        w_copies.append((None, copy))

    core_send(section)
    for k in range(2):
        for peer in space_peers:
            block = slab(f_recv.at[k], peer, rows)
            remote(block, block, f_sems.at[k, 0, 0], f_sems.at[k, 1, peer], "space", peer).wait_recv()
    v_co = (v_a, v_b, v_d)
    for row in range(rows):
        for piece in range(pieces):
            at = pl.ds(row, n_space, stride=rows)
            put(v_co, row, f_recv[0, piece, at, :], f_recv[1, piece, at, :], lanes[piece])

    for at in line:
        for peer in x_peers:
            count_wait(peer, at * 2 + y)
            count_wait(peer, at * 2 + (1 - y))
    for owner in x_peers:
        core_send(owner)

    def spread_counts(owner):
        def one(t, carry):
            for row in range(rows):
                for piece in range(pieces):
                    value = counts[owner, piece, pl.ds(t * rows + row, n_space, stride=own_rows), :]
                    wts[owner * steps + t, row, :, lanes[piece]] = value.astype(F32)
            return carry

        lax.fori_loop(0, steps, one, 0)

    for j, peer in enumerate(space_peers):
        block = slab(l_recv, peer, span)
        remote(block, block, l_sems.at[0, 0], l_sems.at[1, peer], "space", peer).wait_recv()

    def received(row, piece):
        return l_recv[piece, pl.ds(row, n_space, stride=span), :]

    for row in range(rows):
        for piece in range(pieces):
            value = received(halo + row, piece)
            from_below = row - (rows - halo)
            if from_below >= 0:
                value = value + shift_groups(received(from_below, piece), -1)
            if row < halo:
                value = value + shift_groups(received(halo + rows + row, piece), 1)
            resid[row, :, lanes[piece]] = value
            r_send[0, piece, pl.ds(row, n_space, stride=rows), :] = value

    def residual_copy(k, j, peer):
        return remote(
            slab(r_send.at[k], peer, rows),
            slab(r_recv.at[k], place, rows),
            r_sems.at[k, 0, j],
            r_sems.at[k, 1, place],
            "space",
            peer,
        )

    def send_residual(k, first=0, last=n_space - 1):
        for j, peer in list(enumerate(space_peers))[first:last]:
            residual_copy(k, j, peer).start()
        if first:
            return
        slab(r_recv.at[k], place, rows)[...] = slab(r_send.at[k], place, rows)[...]

    def peer_slot(peer):
        return peer["tm"] * n_space + peer["space"]

    me = section * n_space + place

    def reduce_all(k, partials, meanwhile):
        at = lax.broadcasted_iota(jnp.int32, (16, 128), 0)
        lane = lax.broadcasted_iota(jnp.int32, (16, 128), 1)
        tile = jnp.zeros((16, 128), F32)
        for j, partial in enumerate(partials):
            folded = partial[:, lanes[0]]
            for piece in range(1, pieces):
                folded = folded + partial[:, lanes[piece]]
            tile = jnp.where(at == j, jnp.sum(folded, axis=0, keepdims=True), tile)
        tile = jnp.where(at == lane, jnp.sum(tile, axis=1, keepdims=True), 0.0)
        line = jnp.sum(tile, axis=0, keepdims=True)
        red_src[k] = line
        red_recv[k, me] = line
        copies = [
            pltpu.make_async_remote_copy(
                src_ref=red_src.at[k],
                dst_ref=red_recv.at[k, me],
                send_sem=red_sems.at[k, 0, j],
                recv_sem=red_sems.at[k, 1, me],
                device_id=peer,
                device_id_type=MESH,
            )
            for j, peer in enumerate(everyone)
        ]
        for copy in copies:
            copy.start()
        meanwhile()
        for j, peer in enumerate(everyone):
            copies[j].wait_send()
            pltpu.make_async_remote_copy(
                src_ref=red_src.at[k],
                dst_ref=red_recv.at[k, peer_slot(peer)],
                send_sem=red_sems.at[k, 0, j],
                recv_sem=red_sems.at[k, 1, peer_slot(peer)],
                device_id=peer,
                device_id_type=MESH,
            ).wait_recv()
        line = red_recv[k, 0]
        for j in range(1, n_tm * n_space):
            line = line + red_recv[k, j]
        line = jnp.broadcast_to(line, (8, 128))
        lane = lane[:8]
        return [
            jnp.sum(jnp.where(lane == j, line, 0.0), axis=1, keepdims=True)[0:1]
            for j in range(len(partials))
        ]

    adj = [adj_0, adj_1]
    image = adj[(total - 1) % 2]

    def keep_residual(k, row, value):
        for piece in range(pieces):
            r_send[k, piece, pl.ds(row, n_space, stride=rows), :] = value[:, lanes[piece]]

    def scalar(k):
        return steps_ab[k, 0:1, 0:1]

    def set_scalar(k, value):
        steps_ab[k] = jnp.broadcast_to(value, (8, 128))

    def dots(names, vectors):
        sums = [jnp.zeros((n_space, cols), F32)] * len(names)
        for row in range(rows):
            at = vectors(row)
            sums = [total_ + at[pair_[0]] * at[pair_[1]] for total_, pair_ in zip(sums, names)]
        return sums

    def take_counts():
        for owner in (section, *x_peers):
            spread_counts(owner)
        for d_x in range(n_x):
            owner = lax.rem(x + d_x, n_x) * 2 + (1 - core)
            block = counts.at[owner]
            remote(block, block, w_send.at[0], core_recv.at[owner], "tm", core_peer).wait_recv()
            spread_counts(owner)

    def send_first():
        send_residual(0)
        send_residual(1)

    def first_step():
        def vectors(row):
            r = resid[row]
            q = r + image[row]
            q_0[row] = q
            keep_residual(1, row, q)
            return {"r": r, "q": q}

        rr, rq, qq = reduce_all(0, dots(("rr", "rq", "qq"), vectors), send_first)
        alpha = rr / rq
        beta = (rr - 2.0 * alpha * rq + alpha * alpha * qq) / rr
        set_scalar(0, alpha)
        set_scalar(1, beta)
        for row in range(rows):
            r_0 = resid[row]
            r = r_0 - alpha * q_0[row]
            resid[row] = r
            d = r + beta * r_0
            d_1[row] = d
            states[0, row] = d

    def second_image():
        for row in range(rows):
            u = states[0, row] + image[row]
            u_1[row] = u
            states[0, row] = u
            keep_residual(2, row, u)
        send_residual(2, 0, 2)

    def last_steps():
        def vectors(row):
            u = u_1[row]
            v = u + image[row]
            image[row] = v
            return {"r": resid[row], "d": d_1[row], "u": u, "v": v, "q": q_0[row]}

        names = ("rr", "du", "ru", "uu", "rq", "uq", "dq", "rv", "uv", "dv")
        rr, du, ru, uu, rq, uq, dq, rv, uv, dv = reduce_all(
            1, dots(names, vectors), lambda: send_residual(2, 2)
        )
        beta_1 = scalar(1)
        alpha = rr / du
        rr_2 = rr - 2.0 * alpha * ru + alpha * alpha * uu
        beta = rr_2 / rr
        on_u, on_q, on_v = 1.0 + beta, -beta_1, -alpha
        curve = (
            (on_u * ru + on_q * rq + on_v * rv)
            - alpha * (on_u * uu + on_q * uq + on_v * uv)
            + beta * (on_u * du + on_q * dq + on_v * dv)
        )
        alpha_2 = rr_2 / curve
        for row in range(rows):
            u = u_1[row]
            r_2 = resid[row] - alpha * u
            keep_residual(3, row, r_2 - alpha_2 * (on_u * u + on_q * q_0[row] + on_v * image[row]))
        send_residual(3)
        kept = alpha + alpha_2 * beta
        on_r_1 = kept + alpha_2
        set_scalar(2, scalar(0) + kept * beta_1 + on_r_1)
        set_scalar(3, -scalar(0) * on_r_1)
        set_scalar(4, -alpha * alpha_2)

    def one_product(k, carry):
        for t in range(1, total):
            level_forward(states.at[t - 1], states.at[t], v_co)
        pl.when(k == 0)(take_counts)
        for row in range(rows):
            adj_0[row] = wts[total - 1, row] * states[total - 1, row]
        slot = 0
        for t in range(total - 2, -1, -1):
            level_backward(adj[slot], adj[1 - slot], states.at[t], wts.at[t], v_co)
            slot = 1 - slot
        pl.when(k == 0)(first_step)
        pl.when(k == 1)(second_image)
        pl.when(k == 2)(last_steps)
        return carry

    states[0] = resid[...]
    lax.fori_loop(0, ITERS, one_product, 0)

    def residual_arrived(k):
        for peer in space_peers:
            block = slab(r_recv.at[k], peer, rows)
            remote(block, block, r_sems.at[k, 0, 0], r_sems.at[k, 1, peer], "space", peer).wait_recv()

    for k in range(ITERS):
        residual_arrived(k)
    for piece in range(pieces):
        value = steps_ab[2, 0:1, :] * r_recv[0, piece]
        for k in range(1, ITERS):
            value = value + steps_ab[2 + k, 0:1, :] * r_recv[k, piece]
        control[piece] = value
    residual_arrived(ITERS)
    residual[...] = r_recv[ITERS]

    for k in range(ITERS + 1):
        for j, peer in enumerate(space_peers):
            residual_copy(k, j, peer).wait_send()
    for valid, copy in w_copies:
        if valid is None:
            copy.wait_send()
        else:
            pl.when(valid)(copy.wait_send)
    for copy in f_copies + l_copies:
        copy.wait_send()


def assimilate_call(innovations, obs_counts, diffusion, courant, n_space, n_tm):
    steps, levels, fine_rows, fine_cols = innovations.shape
    part = levels // n_tm
    rows, cols = fine_rows // COARSE, fine_cols // COARSE
    pieces = cols // 128
    total = steps * n_tm
    halo = total - 1
    reach = steps - 1
    padded = rows + 2 * (reach + 1)
    ext = rows + 2 * (halo + 1)
    span = -(-(rows + 2 * halo) // 8) * 8
    row = (part, cols)
    n_x, n_z = n_tm // 2, n_space // 2
    sends = 2 + n_x + 2 * (n_z - 1) * (1 + n_x) + n_z * (n_x - 1) + n_x
    dma = pltpu.SemaphoreType.DMA
    shapes = [
        pltpu.VMEM((SLOTS, part, fine_rows, fine_cols), BF16),
        pltpu.VMEM((pieces, part * fine_rows, 128), F32),
        pltpu.VMEM((pieces, part * rows, 128), F32),
        pltpu.VMEM((2, pieces, levels * rows, 128), F32),
        pltpu.VMEM((n_tm, pieces, n_space * steps * rows, 128), jnp.int32),
        pltpu.VMEM((steps, padded, *row), F32),
        pltpu.VMEM((padded, *row), F32),
        pltpu.VMEM((padded, *row), F32),
        pltpu.VMEM((padded, *row), F32),
        pltpu.VMEM((2, padded, *row), F32),
        pltpu.VMEM((n_tm, rows + 2 * reach, *row), F32),
        pltpu.VMEM((n_tm, rows + 2 * reach, *row), F32),
        pltpu.VMEM((2, 2, n_tm, *row), F32),
        pltpu.VMEM((2, 2, n_tm, *row), F32),
        pltpu.VMEM((2, 2, halo - 1, *row), F32),
        pltpu.VMEM((2, 2, halo - 1, *row), F32),
        pltpu.VMEM((ext, *row), F32),
        pltpu.VMEM((ext, *row), F32),
        pltpu.VMEM((ext, *row), F32),
        pltpu.VMEM((ext, *row), F32),
        pltpu.VMEM((ext, *row), F32),
        pltpu.VMEM((pieces, n_space * span, 128), F32),
        pltpu.VMEM((pieces, n_space * span, 128), F32),
        pltpu.VMEM((2, pieces, n_space * rows, 128), F32),
        pltpu.VMEM((rows, n_space, cols), F32),
        pltpu.VMEM((rows, n_space, cols), F32),
        pltpu.VMEM((rows, n_space, cols), F32),
        pltpu.VMEM((total, rows, n_space, cols), F32),
        pltpu.VMEM((total, rows, n_space, cols), F32),
        pltpu.VMEM((rows, n_space, cols), F32),
        pltpu.VMEM((rows, n_space, cols), F32),
        pltpu.VMEM((rows, n_space, cols), F32),
        pltpu.VMEM((rows, n_space, cols), F32),
        pltpu.VMEM((rows, n_space, cols), F32),
        pltpu.VMEM((rows, n_space, cols), F32),
        pltpu.VMEM((ITERS + 1, pieces, n_space * rows, 128), F32),
        pltpu.VMEM((ITERS + 1, pieces, n_space * rows, 128), F32),
        pltpu.VMEM((2, 1, 128), F32),
        pltpu.VMEM((2, n_tm * n_space, 1, 128), F32),
        pltpu.VMEM((5, 8, 128), F32),
        dma((SLOTS,)),
        dma((pieces, 3)),
        dma((sends,)),
        dma((n_tm, n_space)),
        dma((n_tm,)),
        dma((2, 2, 2)),
        dma((2, 2, 2)),
        dma((2, 2, n_space)),
        dma((2, n_tm)),
        dma((2, n_space)),
        dma((ITERS + 1, 2, n_space)),
        dma((2, 2, n_tm * n_space)),
    ]
    out = jax.ShapeDtypeStruct((pieces, part * rows, 128), F32)
    return pl.pallas_call(
        functools.partial(assimilate_kernel, n_space, n_tm),
        out_shape=[out] * 2,
        in_specs=[pl.BlockSpec(memory_space=pl.ANY)] * 4,
        out_specs=[pl.BlockSpec(memory_space=pltpu.VMEM)] * 2,
        scratch_shapes=shapes,
        compiler_params=pltpu.CompilerParams(
            collective_id=0, has_side_effects=True, vmem_limit_bytes=60 * 2**20
        ),
        name="assimilate",
    )(
        innovations,
        obs_counts.reshape(steps * rows, cols),
        diffusion.reshape(levels * rows, cols),
        courant.reshape(levels * rows, cols),
    )


def expand_kernel(control, residual, increment, residual_out, held, passed, repeated, wide_out, in_sems, out_sems):
    pieces, part, rows, _ = control.shape
    wide = 128 * COARSE
    arrive = []
    for k, (src, dst) in enumerate(((control, held), (residual, passed))):
        arrive.append(pltpu.make_async_copy(src, dst, in_sems.at[k]))
        arrive[k].start()
    pick = jnp.where(
        lax.broadcasted_iota(jnp.int32, (256, wide), 1) // COARSE
        == lax.rem(lax.broadcasted_iota(jnp.int32, (256, wide), 0), 128),
        1.0,
        0.0,
    ).astype(BF16)
    leave = []
    arrive[0].wait()
    for level in range(part):
        for piece in range(pieces):
            values = held[piece, level]
            for sub in range(COARSE):
                repeated[level % 2, piece, pl.ds(sub, rows, stride=COARSE), :] = values
            whole = repeated[level % 2, piece]
            head = whole.astype(BF16)
            rest = (whole - head.astype(F32)).astype(BF16)
            both = jnp.concatenate([head, rest], axis=1)
            wide_out[level, :, piece * wide : (piece + 1) * wide] = jnp.dot(
                both, pick, preferred_element_type=F32
            )
        leave.append(
            pltpu.make_async_copy(wide_out.at[level], increment.at[level], out_sems.at[level])
        )
        leave[-1].start()
        if level == 0:
            arrive[1].wait()
            for piece in range(pieces):
                at = pl.ds(piece * 128, 128)
                leave.append(
                    pltpu.make_async_copy(
                        passed.at[piece], residual_out.at[:, :, at], out_sems.at[part + piece]
                    )
                )
                leave[-1].start()
    for copy in leave:
        copy.wait()


def expand_call(control, residual, part):
    pieces, count, _ = control.shape
    rows, cols = count // part, pieces * 128
    fine = (part, rows * COARSE, cols * COARSE)
    cut = (pieces, part, rows, 128)
    dma = pltpu.SemaphoreType.DMA
    return pl.pallas_call(
        expand_kernel,
        in_specs=[pl.BlockSpec(memory_space=pl.ANY)] * 2,
        out_specs=[pl.BlockSpec(memory_space=pl.ANY)] * 2,
        out_shape=[
            jax.ShapeDtypeStruct(fine, F32),
            jax.ShapeDtypeStruct((part, rows, cols), F32),
        ],
        scratch_shapes=[
            pltpu.VMEM(cut, F32),
            pltpu.VMEM(cut, F32),
            pltpu.VMEM((2, pieces, rows * COARSE, 128), F32),
            pltpu.VMEM(fine, F32),
            dma((2,)),
            dma((part + pieces,)),
        ],
        compiler_params=pltpu.CompilerParams(vmem_limit_bytes=67_043_328),
        name="expand",
    )(control.reshape(cut), residual.reshape(cut))


def padded_2(cells, sides, width):
    for axis, dim in sides:
        count = lax.axis_size(axis)
        ends = count - 1
        head = lax.slice_in_dim(cells, 0, width, axis=dim)
        tail = lax.slice_in_dim(cells, cells.shape[dim] - width, cells.shape[dim], axis=dim)
        cells = jnp.concatenate(
            [
                lax.ppermute(tail, axis, [(i, (i + 1) % count) for i in range(ends)]),
                cells,
                lax.ppermute(head, axis, [((i + 1) % count, i) for i in range(ends)]),
            ],
            axis=dim,
        )
    return cells


def laplace_rows(padded, state_field):
    return (
        padded[:, 2:, :]
        + padded[:, :-2, :]
        + jnp.roll(state_field, 1, 2)
        + jnp.roll(state_field, -1, 2)
        - 4.0 * state_field
    )


def tangent(state_field, diffusion, courant):
    padded = padded_2(state_field, (("space", 1),), 1)
    return (
        state_field
        + diffusion * laplace_rows(padded, state_field)
        - courant * (state_field - jnp.roll(state_field, 1, 2))
    )


def adjoint(state_field, diffusion, courant):
    carried = courant * state_field
    spread = diffusion * state_field
    padded = padded_2(spread, (("space", 1),), 1)
    return state_field + laplace_rows(padded, spread) - carried + jnp.roll(carried, -1, 2)


def level_squares(residual):
    return lax.psum(jnp.sum(residual * residual), ("space", "tm"))


def level_curve(direction, hessian_image):
    return lax.psum(jnp.sum(direction * hessian_image), ("space", "tm"))


def solve_inner(rhs_field, hessian_part, norm_fn, curve_fn):
    control = jnp.zeros_like(rhs_field)
    residual = rhs_field
    direction = rhs_field
    norm_now = norm_fn(residual)
    for iter_no in range(ITERS):
        hessian_image = direction + hessian_part(direction)
        step_len = norm_now / curve_fn(direction, hessian_image)
        control = control + step_len * direction
        residual = residual - step_len * hessian_image
        if iter_no + 1 < ITERS:
            norm_next = norm_fn(residual)
            direction = residual + norm_next / norm_now * direction
            norm_now = norm_next
    return (control, residual)


def on_device(innovations, obs_counts, diffusion, courant):
    step_dev = obs_counts.shape[0]
    n_sections = lax.axis_size("tm")
    section_pos = lax.axis_index("tm")
    total_steps = step_dev * n_sections
    weights = obs_counts.astype(jnp.float32)[:, None]
    levels, fine_rows, fine_cols = (
        innovations.shape[1],
        innovations.shape[2],
        innovations.shape[3],
    )
    lev_part = levels // n_sections
    rows, cols = fine_rows // COARSE, fine_cols // COARSE
    n_space = lax.axis_size("space")
    tiled = lev_part == 8 and rows % 8 == 0 and cols % 128 == 0
    paired = n_space == lev_part and n_sections % 2 == 0
    if tiled and paired and rows >= total_steps - 1:
        solved = assimilate_call(innovations, obs_counts, diffusion, courant, n_space, n_sections)
        return tuple(expand_call(*solved, lev_part))
    blocks = innovations.reshape(step_dev, levels, fine_rows // 4, 4, fine_cols // 4, 4).astype(
        jnp.float32
    )
    forcing = weights * jnp.mean(blocks, axis=(3, 5))
    all_weights = lax.all_gather(obs_counts, "tm", axis=0, tiled=True).astype(jnp.float32)[:, None]
    all_forcing = lax.all_to_all(forcing, "tm", split_axis=1, concat_axis=0, tiled=True)
    diff_part = lax.dynamic_slice_in_dim(diffusion, section_pos * lev_part, lev_part, 0)
    cour_part = lax.dynamic_slice_in_dim(courant, section_pos * lev_part, lev_part, 0)

    def level_back(terms):
        current = terms[total_steps - 1]
        for step_no in range(total_steps - 2, -1, -1):
            current = terms[step_no] + adjoint(current, diff_part, cour_part)
        return current

    def level_hess(state_field):
        records = []
        for step_no in range(total_steps):
            records.append(all_weights[step_no] * state_field)
            if step_no + 1 < total_steps:
                state_field = tangent(state_field, diff_part, cour_part)
        return level_back(jnp.stack(records))

    control, residual = solve_inner(level_back(all_forcing), level_hess, level_squares, level_curve)
    increment = jnp.repeat(jnp.repeat(control, 4, axis=1), 4, axis=2)
    return (increment, residual)


def solution(mesh):
    placed = (
        P("tm", None, "space", None),
        P("tm", "space", None),
        P(None, "space", None),
        P(None, "space", None),
    )
    return jax.shard_map(
        on_device,
        mesh=mesh,
        in_specs=placed,
        out_specs=(P("tm", "space", None), P("tm", "space", None)),
        check_vma=False,
    )
```
